32 devices in a mesh: gx: 4 (over y, core), gy: 8 (over z, x).
Axes of the slice: x: 2, y: 2, z: 4, core: 2. Of those that a mesh axis runs over, the one named last changes fastest.
Arguments:
- voxels_fine: bfloat16 [256, 64, 512], P(('gx', 'gy')), may hold values from -6 to 6
- gain_fine: float32 [64], replicated, may hold values from 0.5 to 2
- gain_middle: float32 [128], replicated, may hold values from 0.5 to 2
- gain_coarse: float32 [256], replicated, may hold values from 0.5 to 2
- kernel_fine: bfloat16 [27, 64, 64], replicated, may hold values from -0.15625 to 0.15625
- kernel_middle: bfloat16 [27, 128, 128], replicated, may hold values from -0.109375 to 0.109375
- kernel_coarse: bfloat16 [27, 256, 256], replicated, may hold values from -0.078125 to 0.078125
- lift_middle: bfloat16 [128, 64], replicated, may hold values from -0.75 to 0.75
- lift_coarse: bfloat16 [256, 128], replicated, may hold values from -0.5 to 0.5
- links_fine: int32 [256, 26], P(('gx', 'gy')), may hold values from 0 to 304, as said below
- links_middle: int32 [64, 26], P(('gx', 'gy')), may hold values from 0 to 140, as said below
- links_coarse: int32 [32, 26], P(('gx', 'gy')), may hold values from 0 to 70, as said below
- sends_fine: int32 [32, 256], P(('gx', 'gy')), may hold values from -1 to 47, as said below
- sends_middle: int32 [32, 128], P(('gx', 'gy')), may hold values from -1 to 11, as said below
- sends_coarse: int32 [32, 64], P(('gx', 'gy')), may hold values from -1 to 5, as said below
- parents_middle: int32 [64, 8], P(('gx', 'gy')), may hold values from 0 to 40
- parents_coarse: int32 [32, 8], P(('gx', 'gy')), may hold values from 0 to 34
- uplinks_middle: int32 [32, 32], P(('gx', 'gy')), may hold values from -1 to 7, as said below
- uplinks_coarse: int32 [32, 32], P(('gx', 'gy')), may hold values from -1 to 1, as said below
Outputs:
- output_fine: bfloat16 [256, 64, 512], P(('gx', 'gy'))
- output_middle: bfloat16 [64, 128, 512], P(('gx', 'gy'))
- output_coarse: bfloat16 [32, 256, 512], P(('gx', 'gy'))
The draws below stay inside these ranges and needn't reach their ends.
Inputs may be any that keep to these rules, and one draw needn't show every extreme that they name: `links_fine`: rows 48 and up name received slabs or the zero row of the step. `links_middle`: rows 12 and up name received slabs or the zero row of the step. `links_coarse`: rows 6 and up name received slabs or the zero row of the step. `sends_fine`: -1 marks an empty slot. `sends_middle`: -1 marks an empty slot. `sends_coarse`: -1 marks an empty slot. `uplinks_middle`: -1 marks an empty slot. `uplinks_coarse`: -1 marks an empty slot.
All inputs are finite; a program needn't handle non-finite values.
Results may differ from the reference program's by a relative error of at most 0.015.
Values may be sent and summed in bfloat16 or wider, within the bound.
No kernel may reach another device: no remote copies, remote signals or barrier semaphores. Data moves between devices by JAX's collectives and lax.ppermute only.
A program may use at most 192 MiB of HBM per device.

```python
import math
import jax
import jax.numpy as jnp
from jax import lax

C0 = 64
C1 = 128
C2 = 256
B0_DEV = 8
SLOTS0 = 8
SLOTS1 = 4
SLOTS2 = 2
POOL_SLOTS = 1
B1_DEV = 2
B2_DEV = 1
NB0 = 256
DEVICES = 32


DIRECTIONS = [(along_x, along_y, along_z) for along_x in (-1, 0, 1) for along_y in (-1, 0, 1) for along_z in (-1, 0, 1) if (along_x, along_y, along_z) != (0, 0, 0)]


def face_index(direction):
    for position in range(3):
        if direction[position] != 0:
            return 2 * position + (0 if direction[position] < 0 else 1)
    return 0


def face_ids():
    return jnp.array([face_index(direction) for direction in DIRECTIONS], jnp.int32)


def link_tables(key, bricks, ways, slot_count, remote_pct, stride, offsets, local_width):
    members = DEVICES
    total_rows = members * bricks
    keys = jax.random.split(key, 8)
    device = (jnp.arange(total_rows, dtype=jnp.int32) // bricks)[:, None]
    rolled = jax.random.randint(keys[0], (total_rows, ways), 0, 100)
    nearby = jax.random.randint(keys[1], (total_rows, ways), 1, 5) * (2 * jax.random.randint(keys[2], (total_rows, ways), 0, 2) - 1)
    distant = jax.random.randint(keys[3], (total_rows, ways), 1, members)
    picker = jax.random.randint(keys[4], (total_rows, ways), 0, 100)
    offset = jnp.where(picker < 60, nearby, distant)
    owner = (device + offset + members) % members
    slot = jax.random.randint(keys[5], (total_rows, ways), 0, slot_count)
    local = jax.random.randint(keys[6], (total_rows, ways), 0, local_width // stride) * stride + offsets[None, :]
    remote = rolled < remote_pct
    empty = rolled >= 90
    table = jnp.where(remote, local_width + owner * slot_count + slot, jnp.where(empty, local_width + members * slot_count, local))
    receiver = jnp.broadcast_to(device, (total_rows, ways)).reshape(-1)
    column = (owner * slot_count + slot).reshape(-1)
    usable = jnp.zeros((members, members * slot_count), jnp.int32).at[receiver, column].max(remote.reshape(-1).astype(jnp.int32))
    usable = usable.reshape(members, members, slot_count).transpose(1, 0, 2).reshape(members, members * slot_count)
    chosen = jax.random.randint(keys[7], (members, members * slot_count), 0, local_width)
    senders = jnp.where(usable > 0, chosen, -1)
    return (table.astype(jnp.int32), senders.astype(jnp.int32))


def fine_tables(key):
    return link_tables(jax.random.fold_in(key, 11), B0_DEV, 26, SLOTS0, 60, 6, face_ids(), 6 * B0_DEV)


def middle_tables(key):
    return link_tables(jax.random.fold_in(key, 12), B1_DEV, 26, SLOTS1, 60, 6, face_ids(), 6 * B1_DEV)


def coarse_tables(key):
    return link_tables(jax.random.fold_in(key, 13), B2_DEV, 26, SLOTS2, 88, 6, face_ids(), 6 * B2_DEV)


def middle_parents(key):
    return link_tables(jax.random.fold_in(key, 21), B1_DEV, 8, POOL_SLOTS, 60, 1, jnp.zeros((8,), jnp.int32), B0_DEV)


def coarse_parents(key):
    return link_tables(jax.random.fold_in(key, 22), B2_DEV, 8, POOL_SLOTS, 60, 1, jnp.zeros((8,), jnp.int32), B1_DEV)


def draw_links_fine(key, part):
    return fine_tables(key)[0]


def draw_sends_fine(key, part):
    return fine_tables(key)[1]


def draw_links_middle(key, part):
    return middle_tables(key)[0]


def draw_sends_middle(key, part):
    return middle_tables(key)[1]


def draw_links_coarse(key, part):
    return coarse_tables(key)[0]


def draw_sends_coarse(key, part):
    return coarse_tables(key)[1]


def draw_parents_middle(key, part):
    return middle_parents(key)[0]


def draw_uplinks_middle(key, part):
    return middle_parents(key)[1]


def draw_parents_coarse(key, part):
    return coarse_parents(key)[0]


def draw_uplinks_coarse(key, part):
    return coarse_parents(key)[1]


def level_of(own_key, extent, cuts, low, top_value):
    factor_of, own = 1.0, jax.random.fold_in(own_key, 6)
    for dim, shards_of in cuts:
        draws = jnp.exp(jax.random.uniform(jax.random.fold_in(own, dim), (shards_of,), jnp.float32, low / len(cuts), top_value / len(cuts)))
        factor_of = factor_of * jnp.repeat(draws, extent[dim] // shards_of).reshape([-1 if axis == dim else 1 for axis in range(len(extent))])
    return factor_of


def bell_draw(own_key, shape, deviation, most, cuts=(), held_as=jnp.bfloat16):
    drawn = deviation * jax.random.normal(own_key, shape, jnp.float32)
    if cuts:
        drawn = drawn * level_of(own_key, shape, cuts, -0.22, 0.18)
    return jnp.clip(drawn, -most, most).astype(held_as)


def setup_inputs(seed: int = 0) -> dict:
    key_of = jax.random.split(jax.random.key(seed), 20)
    voxels_fine = bell_draw(key_of[0], (NB0, C0, 512), 1.0, 6.0, ((0, 32),))
    gain_fine = jnp.clip(jnp.exp(jax.random.uniform(key_of[1], (C0,), jnp.float32, math.log(0.5), math.log(2.0))), 0.5, 2.0)
    gain_middle = jnp.clip(jnp.exp(jax.random.uniform(key_of[2], (C1,), jnp.float32, math.log(0.5), math.log(2.0))), 0.5, 2.0)
    gain_coarse = jnp.clip(jnp.exp(jax.random.uniform(key_of[3], (C2,), jnp.float32, math.log(0.5), math.log(2.0))), 0.5, 2.0)
    kernel_fine = bell_draw(key_of[4], (27, C0, C0), (27 * C0) ** -0.5, 0.15625)
    kernel_middle = bell_draw(key_of[5], (27, C1, C1), (27 * C1) ** -0.5, 0.109375)
    kernel_coarse = bell_draw(key_of[6], (27, C2, C2), (27 * C2) ** -0.5, 0.078125)
    lift_middle = bell_draw(key_of[7], (C1, C0), C0 ** -0.5, 0.75)
    lift_coarse = bell_draw(key_of[8], (C2, C1), C1 ** -0.5, 0.5)
    links_fine = draw_links_fine(jax.random.fold_in(key_of[19], 71), 0)
    links_middle = draw_links_middle(jax.random.fold_in(key_of[19], 71), 0)
    links_coarse = draw_links_coarse(jax.random.fold_in(key_of[19], 71), 0)
    sends_fine = draw_sends_fine(jax.random.fold_in(key_of[19], 71), 0)
    sends_middle = draw_sends_middle(jax.random.fold_in(key_of[19], 71), 0)
    sends_coarse = draw_sends_coarse(jax.random.fold_in(key_of[19], 71), 0)
    parents_middle = draw_parents_middle(jax.random.fold_in(key_of[19], 71), 0)
    parents_coarse = draw_parents_coarse(jax.random.fold_in(key_of[19], 71), 0)
    uplinks_middle = draw_uplinks_middle(jax.random.fold_in(key_of[19], 71), 0)
    uplinks_coarse = draw_uplinks_coarse(jax.random.fold_in(key_of[19], 71), 0)
    return dict(voxels_fine=voxels_fine, gain_fine=gain_fine, gain_middle=gain_middle, gain_coarse=gain_coarse, kernel_fine=kernel_fine, kernel_middle=kernel_middle, kernel_coarse=kernel_coarse, lift_middle=lift_middle, lift_coarse=lift_coarse, links_fine=links_fine, links_middle=links_middle, links_coarse=links_coarse, sends_fine=sends_fine, sends_middle=sends_middle, sends_coarse=sends_coarse, parents_middle=parents_middle, parents_coarse=parents_coarse, uplinks_middle=uplinks_middle, uplinks_coarse=uplinks_coarse)


EPSILON = 1e-06
DIRECTIONS = [(along_x, along_y, along_z) for along_x in (-1, 0, 1) for along_y in (-1, 0, 1) for along_z in (-1, 0, 1) if (along_x, along_y, along_z) != (0, 0, 0)]
OFFSETS = [along_x * 100 + along_y * 10 + along_z for along_x in range(3) for along_y in range(3) for along_z in range(3)]

def leading_axis(direction):
    for position in range(3):
        if direction[position] != 0:
            return position
    return 0

def activate(hidden, scales):
    values = hidden.astype(jnp.float32)
    mean_sq = lax.optimization_barrier(jnp.mean(values * values, axis=1, keepdims=True))
    scaled = values * lax.rsqrt(mean_sq + EPSILON) * scales[None, :, None]
    return jax.nn.silu(scaled).astype(jnp.bfloat16)

def brick_faces(active):
    bricks, channels = (active.shape[0], active.shape[1])
    volume = active.reshape(bricks, channels, 8, 8, 8)
    layers = [volume[:, :, 7], volume[:, :, 0], volume[:, :, :, 7], volume[:, :, :, 0], volume[:, :, :, :, 7], volume[:, :, :, :, 0]]
    return jnp.stack(layers, axis=1).reshape(bricks * 6, channels * 64)

def assemble(active, slabs):
    bricks, channels = (active.shape[0], active.shape[1])
    padded = jnp.zeros((bricks, channels, 10, 10, 10), active.dtype)
    padded = padded.at[:, :, 1:9, 1:9, 1:9].set(active.reshape(bricks, channels, 8, 8, 8))
    for placing, direction in enumerate(DIRECTIONS):
        slab_cut = slabs[:, placing].reshape(bricks, channels, 8, 8)
        leading = leading_axis(direction)
        others = [position for position in range(3) if position != leading]
        chosen = tuple((slice(None) if direction[position] == 0 else 7 if direction[position] < 0 else 0 for position in others))
        target = tuple((slice(1, 9) if direction[position] == 0 else 0 if direction[position] < 0 else 9 for position in range(3)))
        padded = padded.at[(slice(None), slice(None)) + target].set(slab_cut[(slice(None), slice(None)) + chosen])
    return padded.reshape(bricks, channels, 1000)

def interior(full):
    bricks, outputs = (full.shape[0], full.shape[1])
    widened = jnp.pad(full, ((0, 0), (0, 0), (0, 22)))
    lattice = widened.reshape(bricks, outputs, 8, 100)[:, :, :, :80].reshape(bricks, outputs, 8, 8, 10)[:, :, :, :, :8]
    return lattice.reshape(bricks, outputs, 512)

def convolve(padded, kernel):
    bricks, channels = (padded.shape[0], padded.shape[1])
    outputs = kernel.shape[1]
    columns = jnp.stack([padded[:, :, offset:offset + 778] for offset in OFFSETS], axis=1).reshape(bricks, 27 * channels, 778)
    flat_kernel = kernel.transpose(1, 0, 2).reshape(outputs, 27 * channels)
    full = jnp.einsum('ok,bkv->bov', flat_kernel.astype(jnp.float32), columns.astype(jnp.float32))
    return interior(full)

def pool_blocks(output):
    bricks, channels = (output.shape[0], output.shape[1])
    values = output.astype(jnp.float32).reshape(bricks, channels, 4, 2, 4, 2, 4, 2)
    return lax.optimization_barrier(jnp.mean(values, axis=(3, 5, 7))).astype(jnp.bfloat16).reshape(bricks, channels * 64)

def place_octants(gathered):
    parents = gathered.shape[0]
    channels = gathered.shape[2] // 64
    volume = gathered.reshape(parents, 2, 2, 2, channels, 4, 4, 4)
    return volume.transpose(0, 4, 1, 5, 2, 6, 3, 7).reshape(parents, channels, 512)

def resolve(link_rows, senders, device, local_width):
    members = senders.shape[0]
    slot_count = senders.shape[1] // members
    is_local = link_rows < local_width
    remote = link_rows - local_width
    is_remote = jnp.logical_and(remote >= 0, remote < members * slot_count)
    bounded = jnp.clip(remote, 0, members * slot_count - 1)
    owner = bounded // slot_count
    picked = senders[owner, device * slot_count + bounded % slot_count]
    global_row = jnp.where(is_local, device * local_width + link_rows, owner * local_width + picked)
    usable = jnp.logical_or(is_local, jnp.logical_and(is_remote, picked >= 0))
    return (jnp.where(usable, global_row, 0).astype(jnp.int32), usable)

def halo_level(hidden, scales, kernel, links, senders):
    members = senders.shape[0]
    bricks = hidden.shape[0] // members
    channels = hidden.shape[1]
    active = lax.map(lambda portion: activate(portion, scales), hidden.reshape(members, bricks, channels, 512)).reshape(hidden.shape)
    faces = brick_faces(active)

    def per_device(device):
        link_rows = lax.dynamic_slice_in_dim(links, device * bricks, bricks, 0)
        global_row, usable = resolve(link_rows, senders, device, 6 * bricks)
        slabs = jnp.where(usable.reshape(-1, 1), jnp.take(faces, global_row.reshape(-1), axis=0), jnp.zeros((), faces.dtype))
        mine = lax.dynamic_slice_in_dim(hidden, device * bricks, bricks, 0)
        mine_active = lax.dynamic_slice_in_dim(active, device * bricks, bricks, 0)
        padded = assemble(mine_active, slabs.reshape(bricks, 26, channels * 64))
        return (mine.astype(jnp.float32) + convolve(padded, kernel)).astype(jnp.bfloat16)
    return lax.map(per_device, jnp.arange(members, dtype=jnp.int32)).reshape(hidden.shape)

def pool_level(output, lift, links, senders):
    members = senders.shape[0]
    children = output.shape[0] // members
    parents = links.shape[0] // members
    channels = output.shape[1]
    blocks = lax.map(pool_blocks, output.reshape(members, children, channels, 512)).reshape(members * children, channels * 64)

    def per_device(device):
        link_rows = lax.dynamic_slice_in_dim(links, device * parents, parents, 0)
        global_row, usable = resolve(link_rows, senders, device, children)
        gathered = jnp.where(usable.reshape(-1, 1), jnp.take(blocks, global_row.reshape(-1), axis=0), jnp.zeros((), blocks.dtype))
        parent_grid = place_octants(gathered.reshape(parents, 8, channels * 64))
        return jnp.einsum('oc,bcv->bov', lift.astype(jnp.float32), parent_grid.astype(jnp.float32)).astype(jnp.bfloat16)
    return lax.map(per_device, jnp.arange(members, dtype=jnp.int32)).reshape(members * parents, lift.shape[0], 512)

def reference(voxels_fine, gain_fine, gain_middle, gain_coarse, kernel_fine, kernel_middle, kernel_coarse, lift_middle, lift_coarse, links_fine, links_middle, links_coarse, sends_fine, sends_middle, sends_coarse, parents_middle, parents_coarse, uplinks_middle, uplinks_coarse):
    output_fine = halo_level(voxels_fine, gain_fine, kernel_fine, links_fine, sends_fine)
    hidden_middle = pool_level(output_fine, lift_middle, parents_middle, uplinks_middle)
    output_middle = halo_level(hidden_middle, gain_middle, kernel_middle, links_middle, sends_middle)
    hidden_coarse = pool_level(output_middle, lift_coarse, parents_coarse, uplinks_coarse)
    output_coarse = halo_level(hidden_coarse, gain_coarse, kernel_coarse, links_coarse, sends_coarse)
    return (output_fine, output_middle, output_coarse)
```

```python
import functools
import jax
import jax.numpy as jnp
import numpy as np
from jax import lax
from jax.experimental import pallas as pl
from jax.experimental.pallas import tpu as pltpu
from jax.sharding import PartitionSpec as P

EPSILON = 1e-06
AXES = ("gx", "gy")
DIRECTIONS = [
    (a, b, c) for a in (-1, 0, 1) for b in (-1, 0, 1) for c in (-1, 0, 1) if (a, b, c) != (0, 0, 0)
]
DIR = {direction: place for place, direction in enumerate(DIRECTIONS)}
WAYS = len(DIRECTIONS)
VMEM = pl.BlockSpec(memory_space=pltpu.VMEM)
SMEM = pl.BlockSpec(memory_space=pltpu.SMEM)
ANY = pl.BlockSpec(memory_space=pl.ANY)
F32 = jnp.float32
BF16 = jnp.bfloat16


def pool_matrix():
    matrix = np.zeros((64, 512), np.float32)
    for x in range(8):
        for y in range(8):
            for z in range(8):
                matrix[(x // 2) * 16 + (y // 2) * 4 + z // 2, x * 64 + y * 8 + z] = 0.125
    return jnp.asarray(matrix, BF16)


def place_matrix():
    matrix = np.zeros((512, 512), np.float32)
    for x in range(8):
        for y in range(8):
            for z in range(8):
                octant = (x // 4) * 4 + (y // 4) * 2 + z // 4
                inner = (x % 4) * 16 + (y % 4) * 4 + z % 4
                matrix[x * 64 + y * 8 + z, octant * 64 + inner] = 1
    return jnp.asarray(matrix, BF16)


def face_matrices():
    matrices = np.zeros((6, 64, 256), np.float32)
    for face in range(6):
        axis, layer = face // 2, 3 if face % 2 == 0 else 0
        for p in range(8):
            for q in range(8):
                inner = [p % 4, q % 4]
                inner.insert(axis, layer)
                octant = (p // 4) * 2 + q // 4
                matrices[face, p * 8 + q, octant * 64 + inner[0] * 16 + inner[1] * 4 + inner[2]] = 1
    return jnp.asarray(matrices, BF16)


def half_masks():
    masks = np.zeros((2, 64, 128), np.float32)
    masks[0, :, :64] = 1
    masks[1, :, 64:] = 1
    return jnp.asarray(masks, BF16)


def silu(v):
    return v / (1.0 + jnp.exp(-v))


def fill_halo(s_ref, e_ref, lo_ref, hi_ref):
    def row(a, b, c):
        return DIR[a, b, c] * 64

    for a, plane in ((-1, 0), (1, 9)):
        base, rim = plane * 80, plane * 16
        e_ref[base + 8 : base + 72] = s_ref[row(a, 0, 0) : row(a, 0, 0) + 64]
        e_ref[base : base + 8] = s_ref[row(a, -1, 0) + 56 : row(a, -1, 0) + 64]
        e_ref[base + 72 : base + 80] = s_ref[row(a, 1, 0) : row(a, 1, 0) + 8]
        for ref, c, at in ((lo_ref, -1, 7), (hi_ref, 1, 0)):
            for y in range(8):
                ref[rim + y : rim + y + 1] = s_ref[row(a, 0, c) + 8 * y + at : row(a, 0, c) + 8 * y + at + 1]
            ref[rim + 8 : rim + 9] = s_ref[row(a, -1, c) + 56 + at : row(a, -1, c) + 57 + at]
            ref[rim + 9 : rim + 10] = s_ref[row(a, 1, c) + at : row(a, 1, c) + at + 1]
    for x in range(8):
        base, rim = (x + 1) * 80, (x + 1) * 16
        e_ref[base : base + 8] = s_ref[row(0, -1, 0) + 8 * x : row(0, -1, 0) + 8 * x + 8]
        e_ref[base + 72 : base + 80] = s_ref[row(0, 1, 0) + 8 * x : row(0, 1, 0) + 8 * x + 8]
        for ref, c, at in ((lo_ref, -1, 7), (hi_ref, 1, 0)):
            ref[rim : rim + 8] = s_ref[row(0, 0, c) + 8 * x : row(0, 0, c) + 8 * x + 8]
            ref[rim + 8 : rim + 9] = s_ref[row(0, -1, c) + 8 * x + at : row(0, -1, c) + 8 * x + at + 1]
            ref[rim + 9 : rim + 10] = s_ref[row(0, 1, c) + 8 * x + at : row(0, 1, c) + 8 * x + at + 1]


def fill_columns(e_ref, lo_ref, hi_ref, p_ref):
    channels = e_ref.shape[1]
    within = lax.broadcasted_iota(jnp.int32, (8, channels), 0)

    def plane(index, carry):
        base = pl.multiple_of(index * 80, 8)
        rim = pl.multiple_of(index * 16, 8)
        into = pl.multiple_of(index * 64, 64)
        shifted = ([], [], [])
        for y in range(10):
            at = 8 if y == 0 else 9 if y == 9 else y - 1
            middle = e_ref[pl.ds(base + 8 * y, 8), :]
            low = jnp.broadcast_to(lo_ref[pl.ds(rim + at, 1), :], (8, channels))
            high = jnp.broadcast_to(hi_ref[pl.ds(rim + at, 1), :], (8, channels))
            shifted[0].append(jnp.where(within == 0, low, pltpu.roll(middle, 1, 0)))
            shifted[1].append(middle)
            shifted[2].append(jnp.where(within == 7, high, pltpu.roll(middle, 7, 0)))
        for dy in range(3):
            for dz in range(3):
                group = jnp.concatenate(shifted[dz][dy : dy + 8], axis=0)
                column = (3 * dy + dz) * channels
                p_ref[pl.ds(into, 64), column : column + channels] = group.astype(BF16)
        return carry

    lax.fori_loop(0, 10, plane, 0)


def contract(p_ref, k_ref):
    total = None
    for dx in range(3):
        part = jnp.dot(p_ref[64 * dx : 64 * dx + 512, :], k_ref[dx], preferred_element_type=F32)
        total = part if total is None else total + part
    return total


def pack_kernel(pairs, slots, sends_ref, x_ref, gain_ref, act_ref, faces_ref, out_ref, a_ref):
    low = lax.broadcasted_iota(jnp.int32, (32, 128), 1) < 64

    def pair(index, carry):
        values = x_ref[pl.ds(2 * index, 2)].astype(F32)
        mean_sq = jnp.mean(values * values, axis=1, keepdims=True)
        scaled = values * lax.rsqrt(mean_sq + EPSILON) * gain_ref[...][None]
        rounded = silu(scaled).astype(BF16).astype(F32).reshape(128, 512)
        a_ref[...] = rounded.T
        act_ref[index] = a_ref[...].astype(BF16)
        for face in range(6):
            axis, at = face // 2, 7 if face % 2 == 0 else 0
            if axis == 0:
                layer = a_ref[64 * at : 64 * at + 64, :]
            elif axis == 1:
                layer = jnp.concatenate(
                    [a_ref[64 * x + 8 * at : 64 * x + 8 * at + 8, :] for x in range(8)], axis=0
                )
            else:
                layer = a_ref[pl.ds(at, 64, stride=8), :]
            first, second = layer[:32], layer[32:]
            faces_ref[12 * index + face] = jnp.where(low, first, pltpu.roll(second, 64, 1)).astype(BF16)
            faces_ref[12 * index + 6 + face] = jnp.where(low, pltpu.roll(first, 64, 1), second).astype(
                BF16
            )
        return carry

    lax.fori_loop(0, pairs, pair, 0)
    empty = 12 * pairs
    faces_ref[empty] = jnp.zeros((32, 128), BF16)

    def slot(index, carry):
        for step in range(8):
            row = sends_ref[0, 8 * index + step]
            out_ref[8 * index + step] = faces_ref[jnp.where(row < 0, empty, row)]
        return carry

    lax.fori_loop(0, slots // 8, slot, 0)


def fine_kernel(
    pairs, links_ref, x_ref, act_ref, faces_ref, arrived_ref, k_ref, pool_ref, out_ref, pooled_ref,
    t_ref, s_ref, e_ref, lo_ref, hi_ref, p_ref,
):
    low = lax.broadcasted_iota(jnp.int32, (32, 128), 1) < 64
    own = 12 * pairs
    received = arrived_ref.shape[0]
    t_ref[0:own] = faces_ref[0:own]
    t_ref[own : own + received] = arrived_ref[...]
    t_ref[own + received] = jnp.zeros((32, 128), BF16)

    def pair(index, carry):
        for way in range(WAYS):
            first = t_ref[links_ref[2 * index, way]].astype(F32)
            second = t_ref[links_ref[2 * index + 1, way]].astype(F32)
            s_ref[64 * way : 64 * way + 32] = jnp.where(low, first, pltpu.roll(second, 64, 1))
            s_ref[64 * way + 32 : 64 * way + 64] = jnp.where(low, pltpu.roll(first, 64, 1), second)
        for x in range(8):
            e_ref[80 * x + 88 : 80 * x + 152] = act_ref[index, 64 * x : 64 * x + 64].astype(F32)
        fill_halo(s_ref, e_ref, lo_ref, hi_ref)
        fill_columns(e_ref, lo_ref, hi_ref, p_ref)
        total = contract(p_ref, k_ref).T
        source = x_ref[pl.ds(2 * index, 2)].astype(F32).reshape(128, 512)
        result = (source + total).astype(BF16)
        out_ref[pl.ds(2 * index, 2)] = result.reshape(2, 64, 512)
        pooled_ref[index] = lax.dot_general(
            pool_ref[...], result, (((1,), (1,)), ((), ())), preferred_element_type=F32
        ).astype(BF16)
        return carry

    lax.fori_loop(0, pairs, pair, 0)


def level_kernel(bricks, halves, pieces, pooled, *refs):
    meta_ref = refs[0]
    piece_refs = refs[1 : 1 + len(pieces)]
    refs = refs[1 + len(pieces) :]
    gain_ref, lift_ref, k_ref, sel_ref, place_ref, pool_ref, mask_ref, out_ref = refs[:8]
    refs = refs[8:]
    if pooled:
        pooled_ref, refs = refs[0], refs[1:]
    t_ref, x_ref, g_ref, s_ref, e_ref, lo_ref, hi_ref, p_ref, sems = refs
    copies = []
    at = 0
    for place, (ref, size) in enumerate(zip(piece_refs, pieces)):
        copies.append(pltpu.make_async_copy(ref, t_ref.at[pl.ds(at, size)], sems.at[place]))
        at += size
    for copy in copies:
        copy.start()
    t_ref[at] = jnp.zeros((64, 128), BF16)
    for copy in copies:
        copy.wait()
    slabs = bricks * WAYS

    def block(code):
        if halves == 1:
            return t_ref[code]
        return t_ref[code // 2] * mask_ref[code % 2]

    def activate(hidden):
        mean_sq = jnp.mean(hidden * hidden, axis=1, keepdims=True)
        return silu(hidden * lax.rsqrt(mean_sq + EPSILON) * gain_ref[...]).astype(BF16).astype(F32)

    def brick(index, carry):
        for octant in range(8):
            x_ref[64 * octant : 64 * octant + 64] = block(meta_ref[0, 5 * slabs + 8 * index + octant])
        grid = jnp.dot(place_ref[...], x_ref[...], preferred_element_type=F32).astype(BF16)
        hidden = jnp.dot(grid, lift_ref[...], preferred_element_type=F32).astype(BF16).astype(F32)
        active = activate(hidden)
        for x in range(8):
            e_ref[80 * x + 88 : 80 * x + 152] = active[64 * x : 64 * x + 64]
        for way in range(WAYS):
            slab = WAYS * index + way
            four = jnp.concatenate([block(meta_ref[0, 4 * slab + m]) for m in range(4)], axis=0)
            face = meta_ref[0, 4 * slabs + slab]
            g_ref[64 * way : 64 * way + 64] = jnp.dot(
                sel_ref[face], four, preferred_element_type=F32
            ).astype(BF16)

        def lifted(part, carry):
            rows = pl.ds(pl.multiple_of(part * 128, 128), 128)
            rim = jnp.dot(g_ref[rows, :], lift_ref[...], preferred_element_type=F32)
            s_ref[rows, :] = activate(rim.astype(BF16).astype(F32))
            return carry

        lax.fori_loop(0, WAYS // 2, lifted, 0)
        fill_halo(s_ref, e_ref, lo_ref, hi_ref)
        fill_columns(e_ref, lo_ref, hi_ref, p_ref)
        result = (hidden + contract(p_ref, k_ref)).astype(BF16)
        out_ref[index] = result.astype(F32).T.astype(BF16)
        if pooled:
            pooled_ref[index] = jnp.dot(pool_ref[...], result, preferred_element_type=F32).astype(BF16)
        return carry

    lax.fori_loop(0, bricks, brick, 0)


def shift_pairs(size, step):
    half = size // 2
    return [(i, (i // 2 - step) % half * 2 + i % 2) for i in range(size)]


def flip_pairs(size):
    return [(i, i ^ 1) for i in range(size)]


def ring_pairs(size, step):
    return [(i, (i - step) % size) for i in range(size)]


def gather_blocks(blocks, nx, ny):
    n = blocks.shape[0]
    half = n // 2
    column = [blocks] + [lax.ppermute(blocks, "gy", shift_pairs(ny, s)) for s in range(1, ny // 2)]
    first = jnp.concatenate([b[:half] for b in column], axis=0)
    second = jnp.concatenate([b[half:] for b in column], axis=0)
    first = jnp.concatenate([first, lax.ppermute(first, "gy", flip_pairs(ny))], axis=0)
    second = jnp.concatenate(
        [second] + [lax.ppermute(second, "gx", shift_pairs(nx, s)) for s in range(1, nx // 2)], axis=0
    )
    here = [first] + [lax.ppermute(first, "gx", shift_pairs(nx, s)) for s in range(1, nx // 2)]
    here += [second, lax.ppermute(second, "gy", flip_pairs(ny))]
    return here + [lax.ppermute(b, "gx", flip_pairs(nx)) for b in here]


def block_place(device, local, n, nx, ny):
    gx, gy = device // ny, device % ny
    mx, my = lax.axis_index("gx"), lax.axis_index("gy")
    half, columns, rows = n // 2, ny // 2, nx // 2
    core = (gx % 2) ^ (mx % 2)
    yi = (gx // 2 - mx // 2) % rows
    xi = (gy % 2) ^ (my % 2)
    zi = (gy // 2 - my // 2) % columns
    size = nx * ny // 2 * half
    first = ((yi * 2 + xi) * columns + zi) * half + local
    second = size + ((xi * rows + yi) * columns + zi) * half + local - half
    return core * 2 * size + jnp.where(local < half, first, second)


def gather_tables(row, nx, ny):
    rows = [row] + [lax.ppermute(row, "gy", ring_pairs(ny, s)) for s in range(1, ny)]
    part = jnp.concatenate(rows, axis=0)
    parts = [part] + [lax.ppermute(part, "gx", ring_pairs(nx, s)) for s in range(1, nx)]
    table = jnp.concatenate(parts, axis=0)
    order = jnp.arange(nx * ny, dtype=jnp.int32)
    gx = (lax.axis_index("gx") + order // ny) % nx
    gy = (lax.axis_index("gy") + order % ny) % ny
    return table, gx * ny + gy


def pick(where, values, axis):
    return jnp.sum(jnp.where(where, values, 0), axis=axis)


def resolve_level(links, sends, parents, uplinks, owner, children, nx, ny, packed):
    members = nx * ny
    me = lax.axis_index("gx") * ny + lax.axis_index("gy")
    bricks = links.shape[0]
    slots = sends.shape[1] // members
    everyone = jnp.arange(members, dtype=jnp.int32)
    up = pick(everyone[None, None, :] == owner[None, :, None], uplinks[:, None, :], 2)
    peer = parents - children
    owed = pick(
        owner[:, None, None, None] == peer[None], up[:, :, None, None], 0
    )
    remote = (peer >= 0) & (peer < members)
    child = jnp.where(
        parents < children,
        owner[:, None, None] * children + parents,
        jnp.where(remote & (owed >= 0), peer * children + owed, -1),
    )
    own = pick((owner == me)[:, None, None], child, 0)
    flat = links.reshape(-1)
    beyond = flat - 6 * bricks
    mine = lax.dynamic_slice_in_dim(sends, me * slots, slots, 1)
    from_device = jnp.where(beyond < 0, me, beyond // slots)
    row = pick(
        (owner[None, :, None] == (beyond // slots)[:, None, None])
        & (jnp.arange(slots, dtype=jnp.int32)[None, None, :] == (beyond % slots)[:, None, None]),
        mine[None],
        (1, 2),
    )
    row = jnp.where(beyond < 0, flat, row)
    usable = (row >= 0) & (beyond < members * slots)
    safe = jnp.where(usable, row, 0)
    face = safe % 6
    eight = pick(
        (owner[None, :, None, None] == from_device[:, None, None, None])
        & (jnp.arange(bricks, dtype=jnp.int32)[None, None, :, None] == (safe // 6)[:, None, None, None]),
        child[None],
        (1, 2),
    )
    side = 1 - face % 2
    m = jnp.arange(4, dtype=jnp.int32)[None, :]
    axis = (face // 2)[:, None]
    octant = jnp.where(
        axis == 0,
        4 * side[:, None] + m,
        jnp.where(axis == 1, 4 * (m // 2) + 2 * side[:, None] + m % 2, 2 * m + side[:, None]),
    )
    four = pick(octant[:, :, None] == jnp.arange(8, dtype=jnp.int32)[None, None, :], eight[:, None, :], 2)
    four = jnp.where(usable[:, None], four, -1)

    def code(block):
        device, local = jnp.maximum(block, 0) // children, jnp.maximum(block, 0) % children
        tiles = children // packed
        place = block_place(device, local // packed, tiles, nx, ny)
        place = jnp.where(block < 0, members * tiles, place)
        return place * packed + jnp.where(block < 0, 0, local % packed)

    return jnp.concatenate([code(four).reshape(-1), face, code(own).reshape(-1)])[None].astype(jnp.int32)


def run_level(meta, pieces, gain, lift, kernel, bricks, halves, pooled, consts):
    channels = lift.shape[1]
    sel, place, pool, masks = consts
    sizes = [piece.shape[0] for piece in pieces]
    outs = [jax.ShapeDtypeStruct((bricks, channels, 512), BF16)]
    if pooled:
        outs.append(jax.ShapeDtypeStruct((bricks, 64, channels), BF16))
    return pl.pallas_call(
        functools.partial(level_kernel, bricks, halves, sizes, pooled),
        out_shape=outs,
        in_specs=[SMEM] + [ANY] * len(pieces) + [VMEM] * 7,
        out_specs=[VMEM] * len(outs),
        scratch_shapes=[
            pltpu.VMEM((sum(sizes) + 1, 64, 128), BF16),
            pltpu.VMEM((512, 128), BF16),
            pltpu.VMEM((64 * WAYS, 128), BF16),
            pltpu.VMEM((64 * WAYS, channels), F32),
            pltpu.VMEM((800, channels), F32),
            pltpu.VMEM((160, channels), F32),
            pltpu.VMEM((160, channels), F32),
            pltpu.VMEM((640, 9 * channels), BF16),
            pltpu.SemaphoreType.DMA((len(pieces),)),
        ],
        name="level" + str(channels),
    )(meta, *pieces, gain[None, :], lift, kernel, sel, place, pool, masks)


def per_device(
    nx, ny,
    voxels_fine, gain_fine, gain_middle, gain_coarse, kernel_fine, kernel_middle, kernel_coarse,
    lift_middle, lift_coarse, links_fine, links_middle, links_coarse, sends_fine, sends_middle,
    sends_coarse, parents_middle, parents_coarse, uplinks_middle, uplinks_coarse,
):
    members = nx * ny
    bricks0, bricks1, bricks2 = voxels_fine.shape[0], links_middle.shape[0], links_coarse.shape[0]
    pairs = bricks0 // 2
    slots = sends_fine.shape[1]
    pool = pool_matrix()

    act, faces, outgoing = pl.pallas_call(
        functools.partial(pack_kernel, pairs, slots),
        out_shape=[
            jax.ShapeDtypeStruct((pairs, 512, 128), BF16),
            jax.ShapeDtypeStruct((12 * pairs + 1, 32, 128), BF16),
            jax.ShapeDtypeStruct((slots, 32, 128), BF16),
        ],
        in_specs=[SMEM, VMEM, VMEM],
        out_specs=[VMEM] * 3,
        scratch_shapes=[pltpu.VMEM((512, 128), F32)],
        name="pack",
    )(sends_fine, voxels_fine, gain_fine[:, None])

    tables = jnp.concatenate(
        [
            sends_middle, parents_middle.reshape(1, -1), uplinks_middle,
            sends_coarse, parents_coarse.reshape(1, -1), uplinks_coarse,
        ],
        axis=1,
    )
    outgoing, tables, kernel_fine, kernel_middle, kernel_coarse = lax.optimization_barrier(
        (outgoing, tables, kernel_fine, kernel_middle, kernel_coarse)
    )
    arrived = lax.all_to_all(outgoing, AXES, split_axis=0, concat_axis=0, tiled=True)

    table, owner = gather_tables(tables, nx, ny)
    ends = np.cumsum(
        [sends_middle.shape[1], 8 * bricks1, members, sends_coarse.shape[1], 8 * bricks2, members]
    )
    sends1, parents1, uplinks1, sends2, parents2, uplinks2 = jnp.split(table, ends[:-1], axis=1)
    meta1 = resolve_level(
        links_middle, sends1, parents1.reshape(members, bricks1, 8), uplinks1, owner, bricks0, nx, ny, 2
    )
    meta2 = resolve_level(
        links_coarse, sends2, parents2.reshape(members, bricks2, 8), uplinks2, owner, bricks1, nx, ny, 1
    )

    def columns(kernel):
        return kernel.transpose(0, 2, 1).reshape(3, 9 * kernel.shape[2], kernel.shape[1])

    turned = kernel_fine.transpose(0, 2, 1)
    blank = jnp.zeros_like(turned)
    kernel0 = jnp.concatenate(
        [jnp.concatenate([turned, blank], axis=2), jnp.concatenate([blank, turned], axis=2)], axis=1
    ).reshape(3, 9 * 128, 128)
    kernel1, kernel2 = columns(kernel_middle), columns(kernel_coarse)
    lift1 = jnp.concatenate([lift_middle.T, lift_middle.T], axis=0)
    lift2 = lift_coarse.T
    arrived, kernel0, kernel1, kernel2, lift1, lift2, meta1, meta2 = lax.optimization_barrier(
        (arrived, kernel0, kernel1, kernel2, lift1, lift2, meta1, meta2)
    )

    output_fine, pooled_fine = pl.pallas_call(
        functools.partial(fine_kernel, pairs),
        out_shape=[
            jax.ShapeDtypeStruct(voxels_fine.shape, BF16),
            jax.ShapeDtypeStruct((pairs, 64, 128), BF16),
        ],
        in_specs=[SMEM] + [VMEM] * 6,
        out_specs=[VMEM] * 2,
        scratch_shapes=[
            pltpu.VMEM((12 * pairs + slots + 1, 32, 128), BF16),
            pltpu.VMEM((64 * WAYS, 128), F32),
            pltpu.VMEM((800, 128), F32),
            pltpu.VMEM((160, 128), F32),
            pltpu.VMEM((160, 128), F32),
            pltpu.VMEM((640, 9 * 128), BF16),
        ],
        name="fine",
    )(links_fine, voxels_fine, act, faces, arrived, kernel0, pool)

    consts = (face_matrices(), place_matrix(), pool, half_masks())
    output_middle, pooled_middle = run_level(
        meta1, gather_blocks(pooled_fine, nx, ny), gain_middle, lift1, kernel1, bricks1, 2, True, consts
    )
    (output_coarse,) = run_level(
        meta2, gather_blocks(pooled_middle, nx, ny), gain_coarse, lift2, kernel2, bricks2, 1, False, consts
    )
    return (output_fine, output_middle, output_coarse)


def solution(mesh):
    nx, ny = mesh.shape["gx"], mesh.shape["gy"]
    split3, split2, whole = P(AXES, None, None), P(AXES, None), P()
    return jax.shard_map(
        functools.partial(per_device, nx, ny),
        mesh=mesh,
        in_specs=(split3,) + (whole,) * 8 + (split2,) * 10,
        out_specs=(split3,) * 3,
        check_vma=False,
    )
```

```python
import functools
import jax
import jax.numpy as jnp
import numpy as np
from jax import lax
from jax.experimental import pallas as pl
from jax.experimental.pallas import tpu as pltpu
from jax.sharding import PartitionSpec as P

EPSILON = 1e-06
AXES = ("gx", "gy")
DIRECTIONS = [
    (a, b, c) for a in (-1, 0, 1) for b in (-1, 0, 1) for c in (-1, 0, 1) if (a, b, c) != (0, 0, 0)
]
DIR = {direction: place for place, direction in enumerate(DIRECTIONS)}
WAYS = len(DIRECTIONS)
VMEM = pl.BlockSpec(memory_space=pltpu.VMEM)
SMEM = pl.BlockSpec(memory_space=pltpu.SMEM)
ANY = pl.BlockSpec(memory_space=pl.ANY)
HBM = pl.BlockSpec(memory_space=pltpu.HBM)
F32 = jnp.float32
BF16 = jnp.bfloat16


def pool_matrix():
    matrix = np.zeros((64, 512), np.float32)
    for x in range(8):
        for y in range(8):
            for z in range(8):
                matrix[(x // 2) * 16 + (y // 2) * 4 + z // 2, x * 64 + y * 8 + z] = 0.125
    return jnp.asarray(matrix, BF16)


def place_matrix():
    matrix = np.zeros((512, 512), np.float32)
    for x in range(8):
        for y in range(8):
            for z in range(8):
                octant = (x // 4) * 4 + (y // 4) * 2 + z // 4
                inner = (x % 4) * 16 + (y % 4) * 4 + z % 4
                matrix[x * 64 + y * 8 + z, octant * 64 + inner] = 1
    return jnp.asarray(matrix, BF16)


def face_matrices():
    matrices = np.zeros((6, 64, 256), np.float32)
    for face in range(6):
        axis, layer = face // 2, 3 if face % 2 == 0 else 0
        for p in range(8):
            for q in range(8):
                inner = [p % 4, q % 4]
                inner.insert(axis, layer)
                octant = (p // 4) * 2 + q // 4
                matrices[face, p * 8 + q, octant * 64 + inner[0] * 16 + inner[1] * 4 + inner[2]] = 1
    return jnp.asarray(matrices, BF16)


def rim_matrices():
    lines = np.zeros((6, 4, 16, 128), np.float32)
    points = np.zeros((6, 4, 16, 64), np.float32)
    for face in range(6):
        axis, layer = face // 2, 3 if face % 2 == 0 else 0

        def inner(p, q):
            cell = [p % 4, q % 4]
            cell.insert(axis, layer)
            return cell[0] * 16 + cell[1] * 4 + cell[2]

        for side, fixed in enumerate((7, 0)):
            for e in range(8):
                lines[face, side, e, (e // 4) * 64 + inner(fixed, e)] = 1
                lines[face, 2 + side, e, (e // 4) * 64 + inner(e, fixed)] = 1
            for other, second in enumerate((7, 0)):
                points[face, 2 * side + other, 0, inner(fixed, second)] = 1
    return jnp.asarray(lines.reshape(24, 16, 128), BF16), jnp.asarray(points.reshape(24, 16, 64), BF16)


def half_masks():
    masks = np.zeros((2, 64, 128), np.float32)
    masks[0, :, :64] = 1
    masks[1, :, 64:] = 1
    return jnp.asarray(masks, BF16)


WHOLE = 65_500_000


def grant(size):
    return pltpu.CompilerParams(vmem_limit_bytes=min(size, WHOLE))


def divide(value, by):
    return lax.shift_right_arithmetic(value, by.bit_length() - 1) if by & (by - 1) == 0 else value // by


def modulo(value, by):
    return value & (by - 1) if by & (by - 1) == 0 else lax.rem(value, by)


def silu(v):
    return v / (1.0 + jnp.exp(-v))


def kind(direction):
    return sum(1 for step in direction if step != 0)


def fixed_at(direction):
    leading = next(axis for axis in range(3) if direction[axis] != 0)
    rest = [direction[axis] for axis in range(3) if axis != leading]
    return [None if step == 0 else 7 if step < 0 else 0 for step in rest]


def full_rows(direction, entry):
    base = DIR[direction] * 64
    if kind(direction) == 1:
        return base + entry
    p, q = fixed_at(direction)
    if kind(direction) == 3:
        return base + 8 * p + q
    return base + (8 * p + entry if q is None else 8 * entry + q)


FACES = [d for d in DIRECTIONS if kind(d) == 1]
EDGES = [d for d in DIRECTIONS if kind(d) == 2]
CORNERS = [d for d in DIRECTIONS if kind(d) == 3]
COMPACT = 64 * len(FACES) + 16 * len(EDGES) + 16 * len(CORNERS)


def compact_base(direction):
    if kind(direction) == 1:
        return 64 * FACES.index(direction)
    if kind(direction) == 2:
        return 64 * len(FACES) + 16 * EDGES.index(direction)
    return 64 * len(FACES) + 16 * len(EDGES) + 16 * CORNERS.index(direction)


def compact_rows(direction, entry):
    return compact_base(direction) + entry


def fill_halo(s_ref, e_ref, lo_ref, hi_ref, rows):
    def take(ref, at, direction, first, count):
        source = rows(direction, first)
        if rows(direction, first + count - 1) == source + count - 1:
            ref[at : at + count] = s_ref[source : source + count]
        else:
            ref[at : at + count] = s_ref[pl.ds(source, count, stride=8), :]

    for a, plane in ((-1, 0), (1, 9)):
        base, rim = plane * 80, plane * 16
        take(e_ref, base + 8, (a, 0, 0), 0, 64)
        take(e_ref, base, (a, -1, 0), 0, 8)
        take(e_ref, base + 72, (a, 1, 0), 0, 8)
        for ref, c in ((lo_ref, -1), (hi_ref, 1)):
            take(ref, rim, (a, 0, c), 0, 8)
            take(ref, rim + 8, (a, -1, c), 0, 1)
            take(ref, rim + 9, (a, 1, c), 0, 1)
    for x in range(8):
        base, rim = (x + 1) * 80, (x + 1) * 16
        take(e_ref, base, (0, -1, 0), 8 * x, 8)
        take(e_ref, base + 72, (0, 1, 0), 8 * x, 8)
        for ref, c in ((lo_ref, -1), (hi_ref, 1)):
            take(ref, rim, (0, 0, c), 8 * x, 8)
            take(ref, rim + 8, (0, -1, c), x, 1)
            take(ref, rim + 9, (0, 1, c), x, 1)


def fill_columns(e_ref, lo_ref, hi_ref, p_ref):
    channels = e_ref.shape[1]
    within = lax.broadcasted_iota(jnp.int32, (8, channels), 0)

    def plane(index, carry):
        base = pl.multiple_of(index * 80, 8)
        rim = pl.multiple_of(index * 16, 8)
        into = pl.multiple_of(index * 64, 64)
        shifted = ([], [], [])
        for y in range(10):
            at = 8 if y == 0 else 9 if y == 9 else y - 1
            middle = e_ref[pl.ds(base + 8 * y, 8), :]
            low = jnp.broadcast_to(lo_ref[pl.ds(rim + at, 1), :], (8, channels))
            high = jnp.broadcast_to(hi_ref[pl.ds(rim + at, 1), :], (8, channels))
            shifted[0].append(jnp.where(within == 0, low, pltpu.roll(middle, 1, 0)))
            shifted[1].append(middle)
            shifted[2].append(jnp.where(within == 7, high, pltpu.roll(middle, 7, 0)))
        for dy in range(3):
            for dz in range(3):
                group = jnp.concatenate(shifted[dz][dy : dy + 8], axis=0)
                column = (3 * dy + dz) * channels
                p_ref[pl.ds(into, 64), column : column + channels] = group.astype(BF16)
        return carry

    lax.fori_loop(0, 10, plane, 0)


def contract(p_ref, k_ref):
    channels = k_ref.shape[2]
    if k_ref.shape[0] == 3:
        rows = jnp.concatenate([p_ref[64 * dx : 64 * dx + 512, :] for dx in range(3)], axis=1)
        return jnp.dot(rows, k_ref[...].reshape(-1, channels), preferred_element_type=F32)
    both = jnp.dot(p_ref[0:576, :], k_ref[0], preferred_element_type=F32)
    last = jnp.dot(p_ref[128:640, :], k_ref[1][:, :128], preferred_element_type=F32)
    return both[0:512, :128] + both[64:576, 128:] + last


def pack_kernel(
    pairs, slots, sends_ref, sends1_ref, sends2_ref, parents1_ref, parents2_ref, uplinks1_ref, uplinks2_ref,
    x_ref, gain_ref, act_ref, faces_ref, out_ref, a_ref,
):
    low = lax.broadcasted_iota(jnp.int32, (32, 128), 1) < 64
    gain = jnp.broadcast_to(gain_ref[...], (128, 64)).T[:, :1][None]

    def pair(index, carry):
        values = x_ref[pl.ds(2 * index, 2)].astype(F32)
        mean_sq = jnp.mean(values * values, axis=1, keepdims=True)
        scaled = values * lax.rsqrt(mean_sq + EPSILON) * gain
        rounded = silu(scaled).astype(BF16).astype(F32).reshape(128, 512)
        a_ref[...] = rounded.T
        act_ref[index] = a_ref[...].astype(BF16)
        for face in range(6):
            axis, at = face // 2, 7 if face % 2 == 0 else 0
            if axis == 0:
                layer = a_ref[64 * at : 64 * at + 64, :]
            elif axis == 1:
                layer = jnp.concatenate(
                    [a_ref[64 * x + 8 * at : 64 * x + 8 * at + 8, :] for x in range(8)], axis=0
                )
            else:
                layer = a_ref[pl.ds(at, 64, stride=8), :]
            first, second = layer[:32], layer[32:]
            faces_ref[12 * index + face] = jnp.where(low, first, pltpu.roll(second, 64, 1)).astype(BF16)
            faces_ref[12 * index + 6 + face] = jnp.where(low, pltpu.roll(first, 64, 1), second).astype(
                BF16
            )
        return carry

    lax.fori_loop(0, pairs, pair, 0)
    empty = 12 * pairs
    faces_ref[empty] = jnp.zeros((32, 128), BF16)

    members, size = out_ref.shape[0], out_ref.shape[1] - 32 * slots
    place = lax.broadcasted_iota(jnp.int32, (size, 128), 0) * 128 + lax.broadcasted_iota(
        jnp.int32, (size, 128), 1
    )
    common = jnp.zeros((size, 128), jnp.int32)
    own_slots = [ref.shape[1] // members for ref in (sends1_ref, sends2_ref)]
    column, sent = 0, []
    for sends, parents, uplinks, count in (
        (sends1_ref, parents1_ref, uplinks1_ref, own_slots[0]),
        (sends2_ref, parents2_ref, uplinks2_ref, own_slots[1]),
    ):
        sent += [(column + k, sends, count, k) for k in range(count)]
        column += count
        for i in range(parents.shape[0] * 8):
            common = jnp.where(place == column, parents[i // 8, i % 8], common)
            column += 1
        for i in range(members):
            common = jnp.where(place == column, uplinks[0, i], common)
            column += 1

    def peer(index, carry):
        for slot in range(slots):
            row = sends_ref[0, slots * index + slot]
            out_ref[index, 32 * slot : 32 * slot + 32] = faces_ref[jnp.where(row < 0, empty, row)]
        table = common
        for at, sends, count, k in sent:
            table = jnp.where(place == at, sends[0, count * index + k], table)
        out_ref[index, 32 * slots : 32 * slots + size] = table.astype(F32).astype(BF16)
        return carry

    lax.fori_loop(0, members, peer, 0)


def fetch(pairs, sems):
    copies = [pltpu.make_async_copy(src, dst, sems.at[i]) for i, (src, dst) in enumerate(pairs)]
    for copy in copies:
        copy.start()
    return copies


def fine_kernel(
    pairs, links_ref, arrived_hbm, faces_hbm, act_hbm, k_hbm, x_hbm, pool_hbm, out_ref, pooled_ref,
    arrived_ref, faces_ref, act_ref, k_ref, x_ref, pool_ref, s_ref, e_ref, lo_ref, hi_ref, p_ref, sems,
):
    copies = fetch(
        [(arrived_hbm, arrived_ref), (faces_hbm, faces_ref), (act_hbm, act_ref), (k_hbm, k_ref), (x_hbm, x_ref), (pool_hbm, pool_ref)], sems
    )
    low = lax.broadcasted_iota(jnp.int32, (32, 128), 1) < 64
    own = 12 * pairs
    slots = arrived_ref.shape[1] // 32
    received = arrived_ref.shape[0] * slots
    copies[0].wait()
    copies[1].wait()

    def slab(row):
        there = (row >= own) & (row < own + received)
        mine = faces_ref[jnp.minimum(row, own)].astype(F32)
        place = jnp.clip(row - own, 0, received - 1)
        peer = divide(place, slots)
        first = pl.multiple_of((place - peer * slots) * 32, 32)
        theirs = arrived_ref[peer, pl.ds(first, 32), :].astype(F32)
        return jnp.where(there, theirs, mine)

    def pair(index, carry):
        for way in range(WAYS):
            first = slab(links_ref[2 * index, way])
            second = slab(links_ref[2 * index + 1, way])
            s_ref[64 * way : 64 * way + 32] = jnp.where(low, first, pltpu.roll(second, 64, 1))
            s_ref[64 * way + 32 : 64 * way + 64] = jnp.where(low, pltpu.roll(first, 64, 1), second)
        fill_halo(s_ref, e_ref, lo_ref, hi_ref, full_rows)

        @pl.when(index == 0)
        def _():
            for copy in copies[2:]:
                copy.wait()

        for x in range(8):
            e_ref[80 * x + 88 : 80 * x + 152] = act_ref[index, 64 * x : 64 * x + 64].astype(F32)
        fill_columns(e_ref, lo_ref, hi_ref, p_ref)
        total = contract(p_ref, k_ref).T
        source = x_ref[pl.ds(2 * index, 2)].astype(F32).reshape(128, 512)
        result = (source + total).astype(BF16)
        out_ref[pl.ds(2 * index, 2)] = result.reshape(2, 64, 512)
        pooled_ref[index] = lax.dot_general(
            pool_ref[...], result, (((1,), (1,)), ((), ())), preferred_element_type=F32
        ).astype(BF16)
        return carry

    lax.fori_loop(0, pairs, pair, 0)


def level_kernel(bricks, members, halves, pieces, pooled, *refs):
    here_ref, links_ref, sends_ref, places_ref, gain_ref = refs[:5]
    refs = refs[5:]
    piece_refs, refs = refs[: len(pieces)], refs[len(pieces) :]
    hbm_refs, refs = refs[:8], refs[8:]
    out_ref, refs = refs[0], refs[1:]
    if pooled:
        pooled_ref, refs = refs[0], refs[1:]
    t_ref, x_ref, g_ref, s_ref, e_ref, lo_ref, hi_ref, p_ref = refs[:8]
    held_refs, sems = refs[8:16], refs[16]
    k_ref, place_ref, sel_ref, lines_ref, points_ref, pool_ref, mask_ref, lift_ref = held_refs
    work, at = [], 0
    for ref, size in zip(piece_refs, pieces):
        work.append((ref, t_ref.at[pl.ds(at, size)]))
        at += size
    copies = fetch(work + list(zip(hbm_refs[1:], held_refs[1:])) + [(hbm_refs[0], k_ref)], sems)
    t_ref[at] = jnp.zeros((64, 128), BF16)
    me = here_ref[0, 0]
    slots = sends_ref.shape[1]

    for copy in copies[:-1]:
        copy.wait()

    def block(code):
        if halves == 1:
            return t_ref[code]
        return t_ref[lax.shift_right_logical(code, 1)] * mask_ref[code & 1]

    def activate(hidden):
        mean_sq = jnp.mean(hidden * hidden, axis=1, keepdims=True)
        return silu(hidden * lax.rsqrt(mean_sq + EPSILON) * gain_ref[...]).astype(BF16).astype(F32)

    def brick(index, carry):
        for octant in range(8):
            x_ref[64 * octant : 64 * octant + 64] = block(places_ref[8 * index + octant, me])
        grid = jnp.dot(place_ref[...], x_ref[...], preferred_element_type=F32).astype(BF16)
        hidden = jnp.dot(grid, lift_ref[...], preferred_element_type=F32).astype(BF16).astype(F32)
        active = activate(hidden)
        for x in range(8):
            e_ref[80 * x + 88 : 80 * x + 152] = active[64 * x : 64 * x + 64]
        for way, direction in enumerate(DIRECTIONS):
            row = links_ref[index, way]
            beyond = row - 6 * bricks
            inside = jnp.clip(beyond, 0, members * slots - 1)
            peer = divide(inside, slots)
            sent = sends_ref[peer, inside - peer * slots]
            device = jnp.where(beyond < 0, me, peer)
            row = jnp.where(beyond < 0, row, sent)
            usable = (row >= 0) & (beyond < members * slots)
            row = jnp.maximum(row, 0)
            source = lax.shift_right_logical(row * 43691, 18)
            face = row - 6 * source
            axis, side = lax.shift_right_logical(face, 1), 1 - (face & 1)

            def part(m):
                high, least = m // 2, m % 2
                octant = jnp.where(
                    axis == 0, 4 * side + m, jnp.where(axis == 1, 4 * high + 2 * side + least, 2 * m + side)
                )
                code = places_ref[8 * source + octant, device]
                return block(jnp.where(usable, code, at * halves))

            base = compact_base(direction)
            p, q = (None, None) if kind(direction) == 1 else fixed_at(direction)
            if kind(direction) == 1:
                tiles, weights, count = [part(m) for m in range(4)], sel_ref[face], 64
            elif kind(direction) == 2:
                if q is None:
                    tiles, variant = [part(2 * (p // 4)), part(2 * (p // 4) + 1)], 0 if p == 7 else 1
                else:
                    tiles, variant = [part(q // 4), part(2 + q // 4)], 2 if q == 7 else 3
                weights, count = lines_ref[4 * face + variant], 16
            else:
                tiles = [part(2 * (p // 4) + q // 4)]
                weights, count = points_ref[4 * face + (0 if p == 7 else 2) + (0 if q == 7 else 1)], 16
            g_ref[base : base + count] = jnp.dot(
                weights, jnp.concatenate(tiles, axis=0), preferred_element_type=F32
            ).astype(BF16)

        def lifted(step, carry):
            rows = pl.ds(pl.multiple_of(step * (COMPACT // 4), 16), COMPACT // 4)
            rim = jnp.dot(g_ref[rows, :], lift_ref[...], preferred_element_type=F32)
            s_ref[rows, :] = activate(rim.astype(BF16).astype(F32))
            return carry

        lax.fori_loop(0, 4, lifted, 0)
        fill_halo(s_ref, e_ref, lo_ref, hi_ref, compact_rows)
        fill_columns(e_ref, lo_ref, hi_ref, p_ref)

        @pl.when(index == 0)
        def _():
            copies[-1].wait()

        result = (hidden + contract(p_ref, k_ref)).astype(BF16)
        out_ref[index] = result.astype(F32).T.astype(BF16)
        if pooled:
            pooled_ref[index] = jnp.dot(pool_ref[...], result, preferred_element_type=F32).astype(BF16)
        return carry

    lax.fori_loop(0, bricks, brick, 0)


def shift_pairs(size, step):
    half = size // 2
    return [(i, (i // 2 - step) % half * 2 + i % 2) for i in range(size)]


def flip_pairs(size):
    return [(i, i ^ 1) for i in range(size)]


def gather_blocks(blocks, nx, ny, beside):
    n = blocks.shape[0]
    half = n // 2
    column = [blocks] + [lax.ppermute(blocks, "gy", shift_pairs(ny, s)) for s in range(1, ny // 2)]
    first = jnp.concatenate([b[:half] for b in column], axis=0)
    second = jnp.concatenate([b[half:] for b in column], axis=0)
    if beside:
        first, second, *beside = lax.optimization_barrier((first, second, *beside))
    first = jnp.concatenate([first, lax.ppermute(first, "gy", flip_pairs(ny))], axis=0)
    second = jnp.concatenate(
        [second] + [lax.ppermute(second, "gx", shift_pairs(nx, s)) for s in range(1, nx // 2)], axis=0
    )
    here = [first] + [lax.ppermute(first, "gx", shift_pairs(nx, s)) for s in range(1, nx // 2)]
    here += [second, lax.ppermute(second, "gy", flip_pairs(ny))]
    return here + [lax.ppermute(b, "gx", flip_pairs(nx)) for b in here], beside


def block_place(device, local, n, nx, ny, mx, my):
    gx = divide(device, ny)
    gy = device - gx * ny
    half, columns, rows = n // 2, ny // 2, nx // 2
    core = (gx & 1) ^ (mx & 1)
    yi = modulo(divide(gx, 2) - divide(mx, 2) + rows, rows)
    xi = (gy & 1) ^ (my & 1)
    zi = modulo(divide(gy, 2) - divide(my, 2) + columns, columns)
    size = nx * ny // 2 * half
    first = ((yi * 2 + xi) * columns + zi) * half + local
    second = size + ((xi * rows + yi) * columns + zi) * half + local - half
    return core * 2 * size + jnp.where(local < half, first, second)


def places_kernel(nx, ny, levels, here_ref, table_ref, *refs):
    members = nx * ny
    mx, my = here_ref[0, 1], here_ref[0, 2]
    places_refs, sends_refs = refs[0::2], refs[1::2]
    column = 0
    for (bricks, slots, children, packed), places_ref, sends_ref in zip(levels, places_refs, sends_refs):
        parent_at, uplink_at = column + slots, column + slots + 8 * bricks
        sends_ref[...] = table_ref[:, column : column + slots]
        column = uplink_at + members
        tiles = children // packed
        parents = table_ref[:, parent_at : parent_at + 8 * bricks].astype(F32).T.astype(jnp.int32)
        uplinks = table_ref[:, uplink_at : uplink_at + members]
        child_of = lax.broadcasted_iota(jnp.int32, (members, members), 0)
        device = lax.broadcasted_iota(jnp.int32, (1, members), 1)
        for place in range(8 * bricks):
            row = parents[place : place + 1]
            peer = row - children
            owed = jnp.sum(jnp.where(child_of == peer, uplinks, 0), axis=0, keepdims=True)
            usable = (peer < 0) | ((peer < members) & (owed >= 0))
            source = jnp.where(peer < 0, device, jnp.clip(peer, 0, members - 1))
            local = jnp.maximum(jnp.where(peer < 0, row, owed), 0)
            where = block_place(source, divide(local, packed), tiles, nx, ny, mx, my)
            places_ref[place : place + 1] = jnp.where(
                usable, where * packed + modulo(local, packed), members * tiles * packed
            )


def run_level(here, links, sends, places, pieces, gain, lift, kernel, members, halves, pooled, consts):
    bricks, channels = links.shape[0], lift.shape[1]
    sizes = [piece.shape[0] for piece in pieces]
    held = [kernel, *consts, lift]
    outs = [jax.ShapeDtypeStruct((bricks, channels, 512), BF16)]
    if pooled:
        outs.append(jax.ShapeDtypeStruct((bricks, 64, channels), BF16))
    return pl.pallas_call(
        functools.partial(level_kernel, bricks, members, halves, sizes, pooled),
        out_shape=outs,
        in_specs=[SMEM] * 4 + [VMEM] + [ANY] * len(pieces) + [HBM] * len(held),
        out_specs=[VMEM] * len(outs),
        scratch_shapes=[
            pltpu.VMEM((sum(sizes) + 1, 64, 128), BF16),
            pltpu.VMEM((512, 128), BF16),
            pltpu.VMEM((COMPACT, 128), BF16),
            pltpu.VMEM((COMPACT, channels), F32),
            pltpu.VMEM((800, channels), F32),
            pltpu.VMEM((160, channels), F32),
            pltpu.VMEM((160, channels), F32),
            pltpu.VMEM((640, 9 * channels), BF16),
            *[pltpu.VMEM(value.shape, value.dtype) for value in held],
            pltpu.SemaphoreType.DMA((len(pieces) + len(held),)),
        ],
        compiler_params=grant(sum(sizes) * 33_000 + channels * 90_000),
        name="level" + str(channels),
    )(here, links, sends, places, gain[None, :], *pieces, *held)


def per_device(
    nx, ny,
    voxels_fine, gain_fine, gain_middle, gain_coarse, kernel_fine, kernel_middle, kernel_coarse,
    lift_middle, lift_coarse, links_fine, links_middle, links_coarse, sends_fine, sends_middle,
    sends_coarse, parents_middle, parents_coarse, uplinks_middle, uplinks_coarse,
):
    members = nx * ny
    bricks0, bricks1, bricks2 = voxels_fine.shape[0], links_middle.shape[0], links_coarse.shape[0]
    pairs = bricks0 // 2
    pool = pool_matrix()

    mx, my = lax.axis_index("gx"), lax.axis_index("gy")
    here = jnp.stack([mx * ny + my, mx, my])[None].astype(jnp.int32)
    assert members + bricks0 <= 256 and 6 * bricks1 <= 256
    width = sum(
        table.shape[-1]
        for table in (sends_middle.reshape(members, -1), sends_coarse.reshape(members, -1), uplinks_middle, uplinks_coarse)
    ) + 8 * (bricks1 + bricks2)
    size = -(-width // 1024) * 8
    slots = sends_fine.shape[1] // members

    act, faces, outgoing = pl.pallas_call(
        functools.partial(pack_kernel, pairs, slots),
        out_shape=[
            jax.ShapeDtypeStruct((pairs, 512, 128), BF16),
            jax.ShapeDtypeStruct((12 * pairs + 1, 32, 128), BF16),
            jax.ShapeDtypeStruct((members, 32 * slots + size, 128), BF16),
        ],
        in_specs=[SMEM] * 7 + [VMEM] * 2,
        out_specs=[VMEM] * 3,
        scratch_shapes=[pltpu.VMEM((512, 128), F32)],
        compiler_params=grant(WHOLE),
        name="pack",
    )(
        sends_fine, sends_middle, sends_coarse, parents_middle, parents_coarse, uplinks_middle, uplinks_coarse,
        voxels_fine, gain_fine[None],
    )

    outgoing, kernel_fine, kernel_middle, kernel_coarse = lax.optimization_barrier(
        (outgoing, kernel_fine, kernel_middle, kernel_coarse)
    )
    arrived = lax.all_to_all(outgoing, AXES, split_axis=0, concat_axis=0, tiled=True)

    slots1, slots2 = sends_middle.shape[1] // members, sends_coarse.shape[1] // members
    levels = ((bricks1, slots1, bricks0, 2), (bricks2, slots2, bricks1, 1))
    def columns(kernel):
        return kernel.transpose(0, 2, 1).reshape(3, 9 * kernel.shape[2], kernel.shape[1])

    def side_by_side(kernel):
        first = jnp.concatenate([kernel[0], kernel[1]], axis=1)
        return jnp.stack([first, jnp.concatenate([kernel[2], jnp.zeros_like(kernel[2])], axis=1)])

    turned = kernel_fine.transpose(0, 2, 1)
    blank = jnp.zeros_like(turned)
    kernel0 = jnp.concatenate(
        [jnp.concatenate([turned, blank], axis=2), jnp.concatenate([blank, turned], axis=2)], axis=1
    ).reshape(3, 9 * 128, 128)
    kernel1, kernel2 = columns(kernel_middle), columns(kernel_coarse)
    kernel0, kernel1 = side_by_side(kernel0), side_by_side(kernel1)
    lift1 = jnp.concatenate([lift_middle.T, lift_middle.T], axis=0)
    lift2 = lift_coarse.T
    arrived, kernel0, kernel1, kernel2, lift1, lift2 = lax.optimization_barrier(
        (arrived, kernel0, kernel1, kernel2, lift1, lift2)
    )

    output_fine, pooled_fine = pl.pallas_call(
        functools.partial(fine_kernel, pairs),
        out_shape=[
            jax.ShapeDtypeStruct(voxels_fine.shape, BF16),
            jax.ShapeDtypeStruct((pairs, 64, 128), BF16),
        ],
        in_specs=[SMEM] + [HBM] * 6,
        out_specs=[VMEM] * 2,
        scratch_shapes=[
            *[pltpu.VMEM(value.shape, value.dtype) for value in (arrived, faces, act, kernel0, voxels_fine, pool)],
            pltpu.VMEM((64 * WAYS, 128), F32),
            pltpu.VMEM((800, 128), F32),
            pltpu.VMEM((160, 128), F32),
            pltpu.VMEM((160, 128), F32),
            pltpu.VMEM((640, 9 * 128), BF16),
            pltpu.SemaphoreType.DMA((6,)),
        ],
        compiler_params=grant(WHOLE),
        name="fine",
    )(links_fine, arrived, faces, act, kernel0, voxels_fine, pool)

    consts = (place_matrix(), face_matrices(), *rim_matrices(), pool, half_masks())
    table = arrived[:, 32 * slots :].reshape(members, -1)[:, :width].astype(F32).astype(jnp.int32)
    places1, here1, places2, here2 = pl.pallas_call(
        functools.partial(places_kernel, nx, ny, levels),
        out_shape=[
            jax.ShapeDtypeStruct(shape, jnp.int32)
            for bricks, slots_, _, _ in levels
            for shape in ((8 * bricks, members), (members, slots_))
        ],
        in_specs=[SMEM, VMEM],
        out_specs=[VMEM] * 4,
        compiler_params=grant(4_000_000),
        name="places",
    )(here, table)
    blocks, (places1, here1, places2, here2) = gather_blocks(
        pooled_fine, nx, ny, (places1, here1, places2, here2)
    )
    output_middle, pooled_middle = run_level(
        here, links_middle, here1, places1, blocks, gain_middle, lift1, kernel1,
        members, 2, True, consts,
    )
    (output_coarse,) = run_level(
        here, links_coarse, here2, places2, gather_blocks(pooled_middle, nx, ny, ())[0], gain_coarse, lift2, kernel2,
        members, 1, False, consts,
    )
    return (output_fine, output_middle, output_coarse)


def solution(mesh):
    nx, ny = mesh.shape["gx"], mesh.shape["gy"]
    split3, split2, whole = P(AXES, None, None), P(AXES, None), P()
    return jax.shard_map(
        functools.partial(per_device, nx, ny),
        mesh=mesh,
        in_specs=(split3,) + (whole,) * 8 + (split2,) * 10,
        out_specs=(split3,) * 3,
        check_vma=False,
    )
```

```python
import functools
import jax
import jax.numpy as jnp
import numpy as np
from jax import lax
from jax.experimental import pallas as pl
from jax.experimental.pallas import tpu as pltpu
from jax.sharding import PartitionSpec as P

EPSILON = 1e-06
AXES = ("gx", "gy")
DIRECTIONS = [
    (a, b, c) for a in (-1, 0, 1) for b in (-1, 0, 1) for c in (-1, 0, 1) if (a, b, c) != (0, 0, 0)
]
DIR = {direction: place for place, direction in enumerate(DIRECTIONS)}
WAYS = len(DIRECTIONS)
VMEM = pl.BlockSpec(memory_space=pltpu.VMEM)
SMEM = pl.BlockSpec(memory_space=pltpu.SMEM)
ANY = pl.BlockSpec(memory_space=pl.ANY)
HBM = pl.BlockSpec(memory_space=pltpu.HBM)
F32 = jnp.float32
BF16 = jnp.bfloat16


def pool_matrix():
    matrix = np.zeros((64, 512), np.float32)
    for x in range(8):
        for y in range(8):
            for z in range(8):
                matrix[(x // 2) * 16 + (y // 2) * 4 + z // 2, x * 64 + y * 8 + z] = 0.125
    return jnp.asarray(matrix, BF16)


def place_matrix():
    matrix = np.zeros((512, 512), np.float32)
    for x in range(8):
        for y in range(8):
            for z in range(8):
                octant = (x // 4) * 4 + (y // 4) * 2 + z // 4
                inner = (x % 4) * 16 + (y % 4) * 4 + z % 4
                matrix[x * 64 + y * 8 + z, octant * 64 + inner] = 1
    return jnp.asarray(matrix, BF16)


def face_matrices():
    matrices = np.zeros((6, 64, 256), np.float32)
    for face in range(6):
        axis, layer = face // 2, 3 if face % 2 == 0 else 0
        for p in range(8):
            for q in range(8):
                inner = [p % 4, q % 4]
                inner.insert(axis, layer)
                octant = (p // 4) * 2 + q // 4
                matrices[face, p * 8 + q, octant * 64 + inner[0] * 16 + inner[1] * 4 + inner[2]] = 1
    return jnp.asarray(matrices, BF16)


def rim_matrices():
    lines = np.zeros((6, 4, 16, 128), np.float32)
    points = np.zeros((6, 4, 16, 64), np.float32)
    for face in range(6):
        axis, layer = face // 2, 3 if face % 2 == 0 else 0

        def inner(p, q):
            cell = [p % 4, q % 4]
            cell.insert(axis, layer)
            return cell[0] * 16 + cell[1] * 4 + cell[2]

        for side, fixed in enumerate((7, 0)):
            for e in range(8):
                lines[face, side, e, (e // 4) * 64 + inner(fixed, e)] = 1
                lines[face, 2 + side, e, (e // 4) * 64 + inner(e, fixed)] = 1
            for other, second in enumerate((7, 0)):
                points[face, 2 * side + other, 0, inner(fixed, second)] = 1
    return jnp.asarray(lines.reshape(24, 16, 128), BF16), jnp.asarray(points.reshape(24, 16, 64), BF16)


def half_masks():
    masks = np.zeros((2, 64, 128), np.float32)
    masks[0, :, :64] = 1
    masks[1, :, 64:] = 1
    return jnp.asarray(masks, BF16)


WHOLE = 65_500_000


def grant(size):
    return pltpu.CompilerParams(vmem_limit_bytes=min(size, WHOLE))


def divide(value, by):
    return lax.shift_right_arithmetic(value, by.bit_length() - 1) if by & (by - 1) == 0 else value // by


def modulo(value, by):
    return value & (by - 1) if by & (by - 1) == 0 else lax.rem(value, by)


def silu(v):
    return v / (1.0 + jnp.exp(-v))


def kind(direction):
    return sum(1 for step in direction if step != 0)


def fixed_at(direction):
    leading = next(axis for axis in range(3) if direction[axis] != 0)
    rest = [direction[axis] for axis in range(3) if axis != leading]
    return [None if step == 0 else 7 if step < 0 else 0 for step in rest]


def full_rows(direction, entry):
    base = DIR[direction] * 64
    if kind(direction) == 1:
        return base + entry
    p, q = fixed_at(direction)
    if kind(direction) == 3:
        return base + 8 * p + q
    return base + (8 * p + entry if q is None else 8 * entry + q)


FACES = [d for d in DIRECTIONS if kind(d) == 1]
EDGES = [d for d in DIRECTIONS if kind(d) == 2]
CORNERS = [d for d in DIRECTIONS if kind(d) == 3]
COMPACT = 64 * len(FACES) + 16 * len(EDGES) + 16 * len(CORNERS)


def compact_base(direction):
    if kind(direction) == 1:
        return 64 * FACES.index(direction)
    if kind(direction) == 2:
        return 64 * len(FACES) + 16 * EDGES.index(direction)
    return 64 * len(FACES) + 16 * len(EDGES) + 16 * CORNERS.index(direction)


def compact_rows(direction, entry):
    return compact_base(direction) + entry


def fill_halo(s_ref, e_ref, lo_ref, hi_ref, rows):
    def take(ref, at, direction, first, count):
        source = rows(direction, first)
        if rows(direction, first + count - 1) == source + count - 1:
            ref[at : at + count] = s_ref[source : source + count]
        else:
            ref[at : at + count] = s_ref[pl.ds(source, count, stride=8), :]

    for a, plane in ((-1, 0), (1, 9)):
        base, rim = plane * 80, plane * 16
        take(e_ref, base + 8, (a, 0, 0), 0, 64)
        take(e_ref, base, (a, -1, 0), 0, 8)
        take(e_ref, base + 72, (a, 1, 0), 0, 8)
        for ref, c in ((lo_ref, -1), (hi_ref, 1)):
            take(ref, rim, (a, 0, c), 0, 8)
            take(ref, rim + 8, (a, -1, c), 0, 1)
            take(ref, rim + 9, (a, 1, c), 0, 1)
    for x in range(8):
        base, rim = (x + 1) * 80, (x + 1) * 16
        take(e_ref, base, (0, -1, 0), 8 * x, 8)
        take(e_ref, base + 72, (0, 1, 0), 8 * x, 8)
        for ref, c in ((lo_ref, -1), (hi_ref, 1)):
            take(ref, rim, (0, 0, c), 8 * x, 8)
            take(ref, rim + 8, (0, -1, c), x, 1)
            take(ref, rim + 9, (0, 1, c), x, 1)


def build_columns(middles, lows, highs, write):
    within = lax.broadcasted_iota(jnp.int32, middles[1].shape, 0)
    shifted = ([], [], [])
    for middle, low, high in zip(middles, lows, highs):
        if middle is None:
            middle = jnp.zeros_like(middles[1])
            for variant in shifted:
                variant.append(middle)
            continue
        before, after = pltpu.roll(middle, 1, 0), pltpu.roll(middle, 7, 0)
        shifted[0].append(jnp.where(within == 0, low, before))
        shifted[1].append(middle)
        shifted[2].append(jnp.where(within == 7, high, after))
    for d in range(3):
        for e in range(3):
            write(3 * d + e, jnp.concatenate(shifted[e][d : d + 8], axis=0).astype(BF16))


def fill_columns(e_ref, lo_ref, hi_ref, p_ref):
    channels = e_ref.shape[1]

    def plane(index, carry):
        base = pl.multiple_of(index * 80, 8)
        rim = pl.multiple_of(index * 16, 8)
        into = pl.multiple_of(index * 64, 64)

        def edge(ref, y):
            at = 8 if y == 0 else 9 if y == 9 else y - 1
            return jnp.broadcast_to(ref[pl.ds(rim + at, 1), :], (8, channels))

        def write(column, window):
            p_ref[pl.ds(into, 64), column * channels : (column + 1) * channels] = window

        build_columns(
            [e_ref[pl.ds(base + 8 * y, 8), :] for y in range(10)],
            [edge(lo_ref, y) for y in range(10)],
            [edge(hi_ref, y) for y in range(10)],
            write,
        )
        return carry

    lax.fori_loop(0, 10, plane, 0)


def contract(p_ref, k_ref):
    channels = k_ref.shape[2]
    if k_ref.shape[0] == 3:
        rows = jnp.concatenate([p_ref[64 * dx : 64 * dx + 512, :] for dx in range(3)], axis=1)
        return jnp.dot(rows, k_ref[...].reshape(-1, channels), preferred_element_type=F32)
    both = jnp.dot(p_ref[0:576, :], k_ref[0], preferred_element_type=F32)
    last = jnp.dot(p_ref[128:640, :], k_ref[1][:, :128], preferred_element_type=F32)
    return both[0:512, :128] + both[64:576, 128:] + last


def pack_kernel(
    pairs, slots, sends_ref, sends1_ref, sends2_ref, parents1_ref, parents2_ref, uplinks1_ref, uplinks2_ref,
    x_ref, gain_ref, act_ref, faces_ref, out_ref, a_ref,
):
    low = lax.broadcasted_iota(jnp.int32, (32, 128), 1) < 64
    gain = jnp.broadcast_to(gain_ref[...], (128, 64)).T[:, :1][None]

    def pair(index, carry):
        values = x_ref[pl.ds(2 * index, 2)].astype(F32)
        mean_sq = jnp.mean(values * values, axis=1, keepdims=True)
        scaled = values * lax.rsqrt(mean_sq + EPSILON) * gain
        rounded = silu(scaled).astype(BF16).astype(F32).reshape(128, 512)
        a_ref[...] = rounded.T
        act_ref[index] = a_ref[...].astype(BF16)
        for face in range(6):
            axis, at = face // 2, 7 if face % 2 == 0 else 0
            if axis == 0:
                layer = a_ref[64 * at : 64 * at + 64, :]
            elif axis == 1:
                layer = jnp.concatenate(
                    [a_ref[64 * x + 8 * at : 64 * x + 8 * at + 8, :] for x in range(8)], axis=0
                )
            else:
                layer = a_ref[pl.ds(at, 64, stride=8), :]
            first, second = layer[:32], layer[32:]
            faces_ref[12 * index + face] = jnp.where(low, first, pltpu.roll(second, 64, 1)).astype(BF16)
            faces_ref[12 * index + 6 + face] = jnp.where(low, pltpu.roll(first, 64, 1), second).astype(
                BF16
            )
        return carry

    lax.fori_loop(0, pairs, pair, 0)
    empty = 12 * pairs
    faces_ref[empty] = jnp.zeros((32, 128), BF16)

    members, size = out_ref.shape[0], out_ref.shape[1] - 32 * slots
    place = lax.broadcasted_iota(jnp.int32, (size, 128), 0) * 128 + lax.broadcasted_iota(
        jnp.int32, (size, 128), 1
    )
    common = jnp.zeros((size, 128), jnp.int32)
    own_slots = [ref.shape[1] // members for ref in (sends1_ref, sends2_ref)]
    column, sent = 0, []
    for sends, parents, uplinks, count in (
        (sends1_ref, parents1_ref, uplinks1_ref, own_slots[0]),
        (sends2_ref, parents2_ref, uplinks2_ref, own_slots[1]),
    ):
        sent += [(column + k, sends, count, k) for k in range(count)]
        column += count
        for i in range(parents.shape[0] * 8):
            common = jnp.where(place == column, parents[i // 8, i % 8], common)
            column += 1
        for i in range(members):
            common = jnp.where(place == column, uplinks[0, i], common)
            column += 1

    def peer(index, carry):
        for slot in range(slots):
            row = sends_ref[0, slots * index + slot]
            out_ref[index, 32 * slot : 32 * slot + 32] = faces_ref[jnp.where(row < 0, empty, row)]
        table = common
        for at, sends, count, k in sent:
            table = jnp.where(place == at, sends[0, count * index + k], table)
        out_ref[index, 32 * slots : 32 * slots + size] = table.astype(F32).astype(BF16)
        return carry

    lax.fori_loop(0, members, peer, 0)


def fetch(pairs, sems):
    copies = [pltpu.make_async_copy(src, dst, sems.at[i]) for i, (src, dst) in enumerate(pairs)]
    for copy in copies:
        copy.start()
    return copies


def inner_kernel(pairs, act_hbm, k_hbm, inner_ref, act_ref, k_ref, e_ref, lo_ref, hi_ref, p_ref, sems):
    copies = fetch([(act_hbm, act_ref), (k_hbm, k_ref)], sems)
    for ref in (e_ref, lo_ref, hi_ref):
        ref[...] = jnp.zeros_like(ref)
    for copy in copies:
        copy.wait()

    def pair(index, carry):
        for x in range(8):
            e_ref[80 * x + 88 : 80 * x + 152] = act_ref[index, 64 * x : 64 * x + 64].astype(F32)
        fill_columns(e_ref, lo_ref, hi_ref, p_ref)
        inner_ref[index] = contract(p_ref, k_ref)
        return carry

    lax.fori_loop(0, pairs, pair, 0)


def fine_kernel(
    pairs, links_ref, arrived_hbm, faces_hbm, inner_hbm, k_hbm, x_hbm, pool_hbm, out_ref, pooled_ref,
    arrived_ref, faces_ref, total_ref, k_ref, x_ref, pool_ref, s_ref, l_ref, r_ref, sems,
):
    copies = fetch(
        [
            (arrived_hbm, arrived_ref), (faces_hbm, faces_ref), (inner_hbm, total_ref), (k_hbm, k_ref),
            (x_hbm, x_ref), (pool_hbm, pool_ref),
        ],
        sems,
    )
    low = lax.broadcasted_iota(jnp.int32, (32, 128), 1) < 64
    own = 12 * pairs
    slots = arrived_ref.shape[1] // 32
    received = arrived_ref.shape[0] * slots
    copies[0].wait()
    copies[1].wait()

    def slab(row, start, count):
        there = (row >= own) & (row < own + received)
        place = jnp.clip(row - own, 0, received - 1)
        peer = divide(place, slots)
        first = pl.multiple_of((place - peer * slots) * 32, 32)
        mine = faces_ref[jnp.minimum(row, own), start : start + count].astype(F32)
        theirs = arrived_ref[peer, pl.ds(first + start, count), :].astype(F32)
        return jnp.where(there, theirs, mine)

    def row_of(direction, entry):
        at = full_rows(direction, entry)
        return jnp.broadcast_to(s_ref[at : at + 1], (8, 128))

    def group(direction, entry):
        at = full_rows(direction, entry)
        return s_ref[at : at + 8]

    def rims(index, carry):
        for way, direction in enumerate(DIRECTIONS):
            rows = [links_ref[2 * index + half, way] for half in range(2)]
            p = None if kind(direction) == 1 else fixed_at(direction)[0]
            if p != 7:
                count = 32 if p is None else 8
                first, second = [slab(row, 0, count) for row in rows]
                s_ref[64 * way : 64 * way + count] = jnp.where(low[:count], first, pltpu.roll(second, 64, 1))
            if p != 0:
                start = 0 if p is None else 24
                first, second = [slab(row, start, 32 - start) for row in rows]
                s_ref[64 * way + 32 + start : 64 * way + 64] = jnp.where(
                    low[start:], pltpu.roll(first, 64, 1), second
                )
        into = pl.multiple_of(index * 64, 64)

        def writer(side):
            def write(column, window):
                l_ref[side, pl.ds(into, 64), column * 128 : column * 128 + 128] = window

            return write

        zeros = jnp.zeros((8, 128), F32)
        for side, step in enumerate((-1, 1)):
            build_columns(
                [group((step, -1, 0), 0)]
                + [group((step, 0, 0), 8 * y) for y in range(8)]
                + [group((step, 1, 0), 0)],
                [row_of((step, -1, -1), 0)]
                + [row_of((step, 0, -1), y) for y in range(8)]
                + [row_of((step, 1, -1), 0)],
                [row_of((step, -1, 1), 0)]
                + [row_of((step, 0, 1), y) for y in range(8)]
                + [row_of((step, 1, 1), 0)],
                writer(side),
            )
            build_columns(
                [None] + [group((0, step, 0), 8 * x) for x in range(8)] + [None],
                [zeros] * 10,
                [zeros] * 10,
                writer(2 + side),
            )
            build_columns(
                [None] + [group((0, 0, step), 8 * x) for x in range(8)] + [None],
                [None] + [row_of((0, -1, step), x) for x in range(8)] + [None],
                [None] + [row_of((0, 1, step), x) for x in range(8)] + [None],
                writer(4 + side),
            )
        return carry

    lax.fori_loop(0, pairs, rims, 0)
    for copy in copies[2:]:
        copy.wait()
    for side in range(6):
        r_ref[side] = jnp.dot(l_ref[side], k_ref[side], preferred_element_type=F32)

    def finish(index, carry):
        def part(side, first, count):
            return r_ref[side, pl.ds(pl.multiple_of(index * 64 + first, 8), count), :]

        total_ref[index, 0:64] += part(0, 0, 64)
        total_ref[index, 448:512] += part(1, 0, 64)
        for x in range(8):
            total_ref[index, 64 * x : 64 * x + 8] += part(2, 8 * x, 8)
            total_ref[index, 64 * x + 56 : 64 * x + 64] += part(3, 8 * x, 8)
        for side, z in ((4, 0), (5, 7)):
            total_ref[index, pl.ds(z, 64, stride=8), :] += part(side, 0, 64)
        source = x_ref[pl.ds(2 * index, 2)].astype(F32).reshape(128, 512)
        result = (source + total_ref[index].T).astype(BF16)
        out_ref[pl.ds(2 * index, 2)] = result.reshape(2, 64, 512)
        pooled_ref[index] = lax.dot_general(
            pool_ref[...], result, (((1,), (1,)), ((), ())), preferred_element_type=F32
        ).astype(BF16)
        return carry

    lax.fori_loop(0, pairs, finish, 0)


def level_kernel(bricks, members, halves, pieces, pooled, *refs):
    here_ref, links_ref, sends_ref, places_ref, gain_ref = refs[:5]
    refs = refs[5:]
    piece_refs, refs = refs[: len(pieces)], refs[len(pieces) :]
    hbm_refs, refs = refs[:8], refs[8:]
    out_ref, refs = refs[0], refs[1:]
    if pooled:
        pooled_ref, refs = refs[0], refs[1:]
    t_ref, x_ref, g_ref, s_ref, e_ref, lo_ref, hi_ref, p_ref = refs[:8]
    held_refs, sems = refs[8:16], refs[16]
    k_ref, place_ref, sel_ref, lines_ref, points_ref, pool_ref, mask_ref, lift_ref = held_refs
    work, at = [], 0
    for ref, size in zip(piece_refs, pieces):
        work.append((ref, t_ref.at[pl.ds(at, size)]))
        at += size
    copies = fetch(work + list(zip(hbm_refs[1:], held_refs[1:])) + [(hbm_refs[0], k_ref)], sems)
    t_ref[at] = jnp.zeros((64, 128), BF16)
    me = here_ref[0, 0]
    slots = sends_ref.shape[1]

    for copy in copies[:-1]:
        copy.wait()

    def block(code):
        if halves == 1:
            return t_ref[code]
        return t_ref[lax.shift_right_logical(code, 1)] * mask_ref[code & 1]

    def activate(hidden):
        mean_sq = jnp.mean(hidden * hidden, axis=1, keepdims=True)
        return silu(hidden * lax.rsqrt(mean_sq + EPSILON) * gain_ref[...]).astype(BF16).astype(F32)

    def brick(index, carry):
        for octant in range(8):
            x_ref[64 * octant : 64 * octant + 64] = block(places_ref[8 * index + octant, me])
        grid = jnp.dot(place_ref[...], x_ref[...], preferred_element_type=F32).astype(BF16)
        hidden = jnp.dot(grid, lift_ref[...], preferred_element_type=F32).astype(BF16).astype(F32)
        active = activate(hidden)
        for x in range(8):
            e_ref[80 * x + 88 : 80 * x + 152] = active[64 * x : 64 * x + 64]
        for way, direction in enumerate(DIRECTIONS):
            row = links_ref[index, way]
            beyond = row - 6 * bricks
            inside = jnp.clip(beyond, 0, members * slots - 1)
            peer = divide(inside, slots)
            sent = sends_ref[peer, inside - peer * slots]
            device = jnp.where(beyond < 0, me, peer)
            row = jnp.where(beyond < 0, row, sent)
            usable = (row >= 0) & (beyond < members * slots)
            row = jnp.maximum(row, 0)
            source = lax.shift_right_logical(row * 43691, 18)
            face = row - 6 * source
            axis, side = lax.shift_right_logical(face, 1), 1 - (face & 1)

            def part(m):
                high, least = m // 2, m % 2
                octant = jnp.where(
                    axis == 0, 4 * side + m, jnp.where(axis == 1, 4 * high + 2 * side + least, 2 * m + side)
                )
                code = places_ref[8 * source + octant, device]
                return block(jnp.where(usable, code, at * halves))

            base = compact_base(direction)
            p, q = (None, None) if kind(direction) == 1 else fixed_at(direction)
            if kind(direction) == 1:
                tiles, weights, count = [part(m) for m in range(4)], sel_ref[face], 64
            elif kind(direction) == 2:
                if q is None:
                    tiles, variant = [part(2 * (p // 4)), part(2 * (p // 4) + 1)], 0 if p == 7 else 1
                else:
                    tiles, variant = [part(q // 4), part(2 + q // 4)], 2 if q == 7 else 3
                weights, count = lines_ref[4 * face + variant], 16
            else:
                tiles = [part(2 * (p // 4) + q // 4)]
                weights, count = points_ref[4 * face + (0 if p == 7 else 2) + (0 if q == 7 else 1)], 16
            g_ref[base : base + count] = jnp.dot(
                weights, jnp.concatenate(tiles, axis=0), preferred_element_type=F32
            ).astype(BF16)

        def lifted(step, carry):
            rows = pl.ds(pl.multiple_of(step * (COMPACT // 4), 16), COMPACT // 4)
            rim = jnp.dot(g_ref[rows, :], lift_ref[...], preferred_element_type=F32)
            s_ref[rows, :] = activate(rim.astype(BF16).astype(F32))
            return carry

        lax.fori_loop(0, 4, lifted, 0)
        fill_halo(s_ref, e_ref, lo_ref, hi_ref, compact_rows)
        fill_columns(e_ref, lo_ref, hi_ref, p_ref)

        @pl.when(index == 0)
        def _():
            copies[-1].wait()

        result = (hidden + contract(p_ref, k_ref)).astype(BF16)
        out_ref[index] = result.astype(F32).T.astype(BF16)
        if pooled:
            pooled_ref[index] = jnp.dot(pool_ref[...], result, preferred_element_type=F32).astype(BF16)
        return carry

    lax.fori_loop(0, bricks, brick, 0)


def shift_pairs(size, step):
    half = size // 2
    return [(i, (i // 2 - step) % half * 2 + i % 2) for i in range(size)]


def flip_pairs(size):
    return [(i, i ^ 1) for i in range(size)]


def gather_blocks(blocks, nx, ny, beside):
    n = blocks.shape[0]
    half = n // 2
    column = [blocks] + [lax.ppermute(blocks, "gy", shift_pairs(ny, s)) for s in range(1, ny // 2)]
    first = jnp.concatenate([b[:half] for b in column], axis=0)
    second = jnp.concatenate([b[half:] for b in column], axis=0)
    if beside:
        first, second, *beside = lax.optimization_barrier((first, second, *beside))
    first = jnp.concatenate([first, lax.ppermute(first, "gy", flip_pairs(ny))], axis=0)
    second = jnp.concatenate(
        [second] + [lax.ppermute(second, "gx", shift_pairs(nx, s)) for s in range(1, nx // 2)], axis=0
    )
    here = [first] + [lax.ppermute(first, "gx", shift_pairs(nx, s)) for s in range(1, nx // 2)]
    here += [second, lax.ppermute(second, "gy", flip_pairs(ny))]
    return here + [lax.ppermute(b, "gx", flip_pairs(nx)) for b in here], beside


def block_place(device, local, n, nx, ny, mx, my):
    gx = divide(device, ny)
    gy = device - gx * ny
    half, columns, rows = n // 2, ny // 2, nx // 2
    core = (gx & 1) ^ (mx & 1)
    yi = modulo(divide(gx, 2) - divide(mx, 2) + rows, rows)
    xi = (gy & 1) ^ (my & 1)
    zi = modulo(divide(gy, 2) - divide(my, 2) + columns, columns)
    size = nx * ny // 2 * half
    first = ((yi * 2 + xi) * columns + zi) * half + local
    second = size + ((xi * rows + yi) * columns + zi) * half + local - half
    return core * 2 * size + jnp.where(local < half, first, second)


def places_kernel(nx, ny, levels, here_ref, table_ref, *refs):
    members = nx * ny
    mx, my = here_ref[0, 1], here_ref[0, 2]
    places_refs, sends_refs = refs[0::2], refs[1::2]
    column = 0
    for (bricks, slots, children, packed), places_ref, sends_ref in zip(levels, places_refs, sends_refs):
        parent_at, uplink_at = column + slots, column + slots + 8 * bricks
        sends_ref[...] = table_ref[:, column : column + slots]
        column = uplink_at + members
        tiles = children // packed
        parents = table_ref[:, parent_at : parent_at + 8 * bricks].astype(F32).T.astype(jnp.int32)
        uplinks = table_ref[:, uplink_at : uplink_at + members]
        child_of = lax.broadcasted_iota(jnp.int32, (members, members), 0)
        device = lax.broadcasted_iota(jnp.int32, (1, members), 1)
        for place in range(8 * bricks):
            row = parents[place : place + 1]
            peer = row - children
            owed = jnp.sum(jnp.where(child_of == peer, uplinks, 0), axis=0, keepdims=True)
            usable = (peer < 0) | ((peer < members) & (owed >= 0))
            source = jnp.where(peer < 0, device, jnp.clip(peer, 0, members - 1))
            local = jnp.maximum(jnp.where(peer < 0, row, owed), 0)
            where = block_place(source, divide(local, packed), tiles, nx, ny, mx, my)
            places_ref[place : place + 1] = jnp.where(
                usable, where * packed + modulo(local, packed), members * tiles * packed
            )


def run_level(here, links, sends, places, pieces, gain, lift, kernel, members, halves, pooled, consts):
    bricks, channels = links.shape[0], lift.shape[1]
    sizes = [piece.shape[0] for piece in pieces]
    held = [kernel, *consts, lift]
    outs = [jax.ShapeDtypeStruct((bricks, channels, 512), BF16)]
    if pooled:
        outs.append(jax.ShapeDtypeStruct((bricks, 64, channels), BF16))
    return pl.pallas_call(
        functools.partial(level_kernel, bricks, members, halves, sizes, pooled),
        out_shape=outs,
        in_specs=[SMEM] * 4 + [VMEM] + [ANY] * len(pieces) + [HBM] * len(held),
        out_specs=[VMEM] * len(outs),
        scratch_shapes=[
            pltpu.VMEM((sum(sizes) + 1, 64, 128), BF16),
            pltpu.VMEM((512, 128), BF16),
            pltpu.VMEM((COMPACT, 128), BF16),
            pltpu.VMEM((COMPACT, channels), F32),
            pltpu.VMEM((800, channels), F32),
            pltpu.VMEM((160, channels), F32),
            pltpu.VMEM((160, channels), F32),
            pltpu.VMEM((640, 9 * channels), BF16),
            *[pltpu.VMEM(value.shape, value.dtype) for value in held],
            pltpu.SemaphoreType.DMA((len(pieces) + len(held),)),
        ],
        compiler_params=grant(sum(sizes) * 33_000 + channels * 90_000),
        name="level" + str(channels),
    )(here, links, sends, places, gain[None, :], *pieces, *held)


def per_device(
    nx, ny,
    voxels_fine, gain_fine, gain_middle, gain_coarse, kernel_fine, kernel_middle, kernel_coarse,
    lift_middle, lift_coarse, links_fine, links_middle, links_coarse, sends_fine, sends_middle,
    sends_coarse, parents_middle, parents_coarse, uplinks_middle, uplinks_coarse,
):
    members = nx * ny
    bricks0, bricks1, bricks2 = voxels_fine.shape[0], links_middle.shape[0], links_coarse.shape[0]
    pairs = bricks0 // 2
    pool = pool_matrix()

    mx, my = lax.axis_index("gx"), lax.axis_index("gy")
    here = jnp.stack([mx * ny + my, mx, my])[None].astype(jnp.int32)
    assert members + bricks0 <= 256 and 6 * bricks1 <= 256
    width = sum(
        table.shape[-1]
        for table in (sends_middle.reshape(members, -1), sends_coarse.reshape(members, -1), uplinks_middle, uplinks_coarse)
    ) + 8 * (bricks1 + bricks2)
    size = -(-width // 1024) * 8
    slots = sends_fine.shape[1] // members

    act, faces, outgoing = pl.pallas_call(
        functools.partial(pack_kernel, pairs, slots),
        out_shape=[
            jax.ShapeDtypeStruct((pairs, 512, 128), BF16),
            jax.ShapeDtypeStruct((12 * pairs + 1, 32, 128), BF16),
            jax.ShapeDtypeStruct((members, 32 * slots + size, 128), BF16),
        ],
        in_specs=[SMEM] * 7 + [VMEM] * 2,
        out_specs=[VMEM] * 3,
        scratch_shapes=[pltpu.VMEM((512, 128), F32)],
        compiler_params=grant(WHOLE),
        name="pack",
    )(
        sends_fine, sends_middle, sends_coarse, parents_middle, parents_coarse, uplinks_middle, uplinks_coarse,
        voxels_fine, gain_fine[None],
    )

    outgoing, act, kernel_fine, kernel_middle, kernel_coarse = lax.optimization_barrier(
        (outgoing, act, kernel_fine, kernel_middle, kernel_coarse)
    )
    arrived = lax.all_to_all(outgoing, AXES, split_axis=0, concat_axis=0, tiled=True)

    slots1, slots2 = sends_middle.shape[1] // members, sends_coarse.shape[1] // members
    levels = ((bricks1, slots1, bricks0, 2), (bricks2, slots2, bricks1, 1))
    def columns(kernel):
        return kernel.transpose(0, 2, 1).reshape(3, 9 * kernel.shape[2], kernel.shape[1])

    def side_by_side(kernel):
        first = jnp.concatenate([kernel[0], kernel[1]], axis=1)
        return jnp.stack([first, jnp.concatenate([kernel[2], jnp.zeros_like(kernel[2])], axis=1)])

    turned = kernel_fine.transpose(0, 2, 1)
    blank = jnp.zeros_like(turned)
    kernel0 = jnp.concatenate(
        [jnp.concatenate([turned, blank], axis=2), jnp.concatenate([blank, turned], axis=2)], axis=1
    ).reshape(3, 9 * 128, 128)
    kernel1, kernel2 = columns(kernel_middle), columns(kernel_coarse)
    kernel1 = side_by_side(kernel1)
    lift1 = jnp.concatenate([lift_middle.T, lift_middle.T], axis=0)
    lift2 = lift_coarse.T
    cube = kernel0.reshape(3, 3, 3, 128, 128)
    rim0 = jnp.stack(
        [part.reshape(9 * 128, 128) for at in ((0,), (slice(None), 0), (slice(None), slice(None), 0))
         for part in (cube[at], cube[at[:-1] + (2,)])]
    )
    inner = pl.pallas_call(
        functools.partial(inner_kernel, pairs),
        out_shape=jax.ShapeDtypeStruct((pairs, 512, 128), F32),
        in_specs=[HBM] * 2,
        out_specs=VMEM,
        scratch_shapes=[
            pltpu.VMEM(act.shape, BF16),
            pltpu.VMEM((2, 9 * 128, 256), BF16),
            pltpu.VMEM((800, 128), F32),
            pltpu.VMEM((160, 128), F32),
            pltpu.VMEM((160, 128), F32),
            pltpu.VMEM((640, 9 * 128), BF16),
            pltpu.SemaphoreType.DMA((2,)),
        ],
        compiler_params=grant(WHOLE),
        name="inner",
    )(act, side_by_side(kernel0))
    arrived, inner, rim0, kernel1, kernel2, lift1, lift2 = lax.optimization_barrier(
        (arrived, inner, rim0, kernel1, kernel2, lift1, lift2)
    )

    output_fine, pooled_fine = pl.pallas_call(
        functools.partial(fine_kernel, pairs),
        out_shape=[
            jax.ShapeDtypeStruct(voxels_fine.shape, BF16),
            jax.ShapeDtypeStruct((pairs, 64, 128), BF16),
        ],
        in_specs=[SMEM] + [HBM] * 6,
        out_specs=[VMEM] * 2,
        scratch_shapes=[
            *[pltpu.VMEM(value.shape, value.dtype) for value in (arrived, faces, inner, rim0, voxels_fine, pool)],
            pltpu.VMEM((64 * WAYS, 128), F32),
            pltpu.VMEM((6, 64 * pairs, 9 * 128), BF16),
            pltpu.VMEM((6, 64 * pairs, 128), F32),
            pltpu.SemaphoreType.DMA((6,)),
        ],
        compiler_params=grant(WHOLE),
        name="fine",
    )(links_fine, arrived, faces, inner, rim0, voxels_fine, pool)

    consts = (place_matrix(), face_matrices(), *rim_matrices(), pool, half_masks())
    table = arrived[:, 32 * slots :].reshape(members, -1)[:, :width].astype(F32).astype(jnp.int32)
    places1, here1, places2, here2 = pl.pallas_call(
        functools.partial(places_kernel, nx, ny, levels),
        out_shape=[
            jax.ShapeDtypeStruct(shape, jnp.int32)
            for bricks, slots_, _, _ in levels
            for shape in ((8 * bricks, members), (members, slots_))
        ],
        in_specs=[SMEM, VMEM],
        out_specs=[VMEM] * 4,
        compiler_params=grant(4_000_000),
        name="places",
    )(here, table)
    blocks, (places1, here1, places2, here2) = gather_blocks(
        pooled_fine, nx, ny, (places1, here1, places2, here2)
    )
    output_middle, pooled_middle = run_level(
        here, links_middle, here1, places1, blocks, gain_middle, lift1, kernel1,
        members, 2, True, consts,
    )
    (output_coarse,) = run_level(
        here, links_coarse, here2, places2, gather_blocks(pooled_middle, nx, ny, ())[0], gain_coarse, lift2, kernel2,
        members, 1, False, consts,
    )
    return (output_fine, output_middle, output_coarse)


def solution(mesh):
    nx, ny = mesh.shape["gx"], mesh.shape["gy"]
    split3, split2, whole = P(AXES, None, None), P(AXES, None), P()
    return jax.shard_map(
        functools.partial(per_device, nx, ny),
        mesh=mesh,
        in_specs=(split3,) + (whole,) * 8 + (split2,) * 10,
        out_specs=(split3,) * 3,
        check_vma=False,
    )
```

```python
import functools
import jax
import jax.numpy as jnp
import numpy as np
from jax import lax
from jax.experimental import pallas as pl
from jax.experimental.pallas import tpu as pltpu
from jax.sharding import PartitionSpec as P

EPSILON = 1e-06
AXES = ("gx", "gy")
DIRECTIONS = [
    (a, b, c) for a in (-1, 0, 1) for b in (-1, 0, 1) for c in (-1, 0, 1) if (a, b, c) != (0, 0, 0)
]
DIR = {direction: place for place, direction in enumerate(DIRECTIONS)}
WAYS = len(DIRECTIONS)
VMEM = pl.BlockSpec(memory_space=pltpu.VMEM)
SMEM = pl.BlockSpec(memory_space=pltpu.SMEM)
ANY = pl.BlockSpec(memory_space=pl.ANY)
HBM = pl.BlockSpec(memory_space=pltpu.HBM)
F32 = jnp.float32
BF16 = jnp.bfloat16


def pool_matrix():
    matrix = np.zeros((64, 512), np.float32)
    for x in range(8):
        for y in range(8):
            for z in range(8):
                matrix[(x // 2) * 16 + (y // 2) * 4 + z // 2, x * 64 + y * 8 + z] = 0.125
    return jnp.asarray(matrix, BF16)


def place_matrix():
    matrix = np.zeros((512, 512), np.float32)
    for x in range(8):
        for y in range(8):
            for z in range(8):
                octant = (x // 4) * 4 + (y // 4) * 2 + z // 4
                inner = (x % 4) * 16 + (y % 4) * 4 + z % 4
                matrix[x * 64 + y * 8 + z, octant * 64 + inner] = 1
    return jnp.asarray(matrix, BF16)


def face_matrices():
    matrices = np.zeros((6, 64, 256), np.float32)
    for face in range(6):
        axis, layer = face // 2, 3 if face % 2 == 0 else 0
        for p in range(8):
            for q in range(8):
                inner = [p % 4, q % 4]
                inner.insert(axis, layer)
                octant = (p // 4) * 2 + q // 4
                matrices[face, p * 8 + q, octant * 64 + inner[0] * 16 + inner[1] * 4 + inner[2]] = 1
    return jnp.asarray(matrices, BF16)


def rim_matrices():
    lines = np.zeros((6, 4, 16, 128), np.float32)
    points = np.zeros((6, 4, 16, 64), np.float32)
    for face in range(6):
        axis, layer = face // 2, 3 if face % 2 == 0 else 0

        def inner(p, q):
            cell = [p % 4, q % 4]
            cell.insert(axis, layer)
            return cell[0] * 16 + cell[1] * 4 + cell[2]

        for side, fixed in enumerate((7, 0)):
            for e in range(8):
                lines[face, side, e, (e // 4) * 64 + inner(fixed, e)] = 1
                lines[face, 2 + side, e, (e // 4) * 64 + inner(e, fixed)] = 1
            for other, second in enumerate((7, 0)):
                points[face, 2 * side + other, 0, inner(fixed, second)] = 1
    return jnp.asarray(lines.reshape(24, 16, 128), BF16), jnp.asarray(points.reshape(24, 16, 64), BF16)


def half_masks():
    masks = np.zeros((2, 64, 128), np.float32)
    masks[0, :, :64] = 1
    masks[1, :, 64:] = 1
    return jnp.asarray(masks, BF16)


WHOLE = 65_500_000


def grant(size):
    return pltpu.CompilerParams(vmem_limit_bytes=min(size, WHOLE))


def divide(value, by):
    return lax.shift_right_arithmetic(value, by.bit_length() - 1) if by & (by - 1) == 0 else value // by


def modulo(value, by):
    return value & (by - 1) if by & (by - 1) == 0 else lax.rem(value, by)


def fetch(pairs, sems):
    copies = [pltpu.make_async_copy(src, dst, sems.at[i]) for i, (src, dst) in enumerate(pairs)]
    for copy in copies:
        copy.start()
    return copies


def silu(v):
    return v / (1.0 + jnp.exp(-v))


def kind(direction):
    return sum(1 for step in direction if step != 0)


def fixed_at(direction):
    leading = next(axis for axis in range(3) if direction[axis] != 0)
    rest = [direction[axis] for axis in range(3) if axis != leading]
    return [None if step == 0 else 7 if step < 0 else 0 for step in rest]


def full_rows(direction, entry):
    base = DIR[direction] * 64
    if kind(direction) == 1:
        return base + entry
    p, q = fixed_at(direction)
    if kind(direction) == 3:
        return base + 8 * p + q
    return base + (8 * p + entry if q is None else 8 * entry + q)


FACES = [d for d in DIRECTIONS if kind(d) == 1]
EDGES = [d for d in DIRECTIONS if kind(d) == 2]
CORNERS = [d for d in DIRECTIONS if kind(d) == 3]
COMPACT = 64 * len(FACES) + 16 * len(EDGES) + 16 * len(CORNERS)


def compact_base(direction):
    if kind(direction) == 1:
        return 64 * FACES.index(direction)
    if kind(direction) == 2:
        return 64 * len(FACES) + 16 * EDGES.index(direction)
    return 64 * len(FACES) + 16 * len(EDGES) + 16 * CORNERS.index(direction)


def compact_rows(direction, entry):
    return compact_base(direction) + entry


def fill_halo(s_ref, e_ref, lo_ref, hi_ref, rows):
    def take(ref, at, direction, first, count):
        source = rows(direction, first)
        if rows(direction, first + count - 1) == source + count - 1:
            ref[at : at + count] = s_ref[source : source + count]
        else:
            ref[at : at + count] = s_ref[pl.ds(source, count, stride=8), :]

    for a, plane in ((-1, 0), (1, 9)):
        base, rim = plane * 80, plane * 16
        take(e_ref, base + 8, (a, 0, 0), 0, 64)
        take(e_ref, base, (a, -1, 0), 0, 8)
        take(e_ref, base + 72, (a, 1, 0), 0, 8)
        for ref, c in ((lo_ref, -1), (hi_ref, 1)):
            take(ref, rim, (a, 0, c), 0, 8)
            take(ref, rim + 8, (a, -1, c), 0, 1)
            take(ref, rim + 9, (a, 1, c), 0, 1)
    for x in range(8):
        base, rim = (x + 1) * 80, (x + 1) * 16
        take(e_ref, base, (0, -1, 0), 8 * x, 8)
        take(e_ref, base + 72, (0, 1, 0), 8 * x, 8)
        for ref, c in ((lo_ref, -1), (hi_ref, 1)):
            take(ref, rim, (0, 0, c), 8 * x, 8)
            take(ref, rim + 8, (0, -1, c), x, 1)
            take(ref, rim + 9, (0, 1, c), x, 1)


def build_columns(middles, lows, highs, write):
    within = lax.broadcasted_iota(jnp.int32, middles[1].shape, 0)
    shifted = ([], [], [])
    for middle, low, high in zip(middles, lows, highs):
        if middle is None:
            middle = jnp.zeros_like(middles[1])
            for variant in shifted:
                variant.append(middle)
            continue
        before, after = pltpu.roll(middle, 1, 0), pltpu.roll(middle, 7, 0)
        shifted[0].append(jnp.where(within == 0, low, before))
        shifted[1].append(middle)
        shifted[2].append(jnp.where(within == 7, high, after))
    for d in range(3):
        for e in range(3):
            write(3 * d + e, jnp.concatenate(shifted[e][d : d + 8], axis=0).astype(BF16))


def fill_columns(e_ref, lo_ref, hi_ref, p_ref):
    channels = e_ref.shape[1]

    def plane(index, carry):
        base = pl.multiple_of(index * 80, 8)
        rim = pl.multiple_of(index * 16, 8)
        into = pl.multiple_of(index * 64, 64)

        def edge(ref, y):
            at = 8 if y == 0 else 9 if y == 9 else y - 1
            return jnp.broadcast_to(ref[pl.ds(rim + at, 1), :], (8, channels))

        def write(column, window):
            p_ref[pl.ds(into, 64), column * channels : (column + 1) * channels] = window

        build_columns(
            [e_ref[pl.ds(base + 8 * y, 8), :] for y in range(10)],
            [edge(lo_ref, y) for y in range(10)],
            [edge(hi_ref, y) for y in range(10)],
            write,
        )
        return carry

    lax.fori_loop(0, 10, plane, 0)


def contract(p_ref, k_ref):
    channels = k_ref.shape[2]
    if k_ref.shape[0] == 3:
        rows = jnp.concatenate([p_ref[64 * dx : 64 * dx + 512, :] for dx in range(3)], axis=1)
        return jnp.dot(rows, k_ref[...].reshape(-1, channels), preferred_element_type=F32)
    both = jnp.dot(p_ref[0:576, :], k_ref[0], preferred_element_type=F32)
    last = jnp.dot(p_ref[128:640, :], k_ref[1][:, :128], preferred_element_type=F32)
    return both[0:512, :128] + both[64:576, 128:] + last


def pack_kernel(
    pairs, slots, *refs,
):
    index_hbm, (x_hbm, gain_ref, act_hbm, faces_hbm, out_hbm), refs = refs[:7], refs[7:12], refs[12:]
    index_refs, (x_ref, act_ref, faces_ref, out_ref, a_ref, sems, out_sems, late_sems) = refs[:7], refs[7:]
    sends_ref, sends1_ref, sends2_ref, parents1_ref, parents2_ref, uplinks1_ref, uplinks2_ref = index_refs
    copies = fetch([(x_hbm, x_ref), *zip(index_hbm, index_refs)], sems)
    low = lax.broadcasted_iota(jnp.int32, (32, 128), 1) < 64
    gain = jnp.broadcast_to(gain_ref[...], (128, 64)).T[:, :1][None]
    copies[0].wait()

    def pair(index, carry):
        values = x_ref[pl.ds(2 * index, 2)].astype(F32)
        mean_sq = jnp.mean(values * values, axis=1, keepdims=True)
        scaled = values * lax.rsqrt(mean_sq + EPSILON) * gain
        rounded = silu(scaled).astype(BF16).astype(F32).reshape(128, 512)
        a_ref[...] = rounded.T
        act_ref[index] = a_ref[...].astype(BF16)
        for face in range(6):
            axis, at = face // 2, 7 if face % 2 == 0 else 0
            if axis == 0:
                layer = a_ref[64 * at : 64 * at + 64, :]
            elif axis == 1:
                layer = jnp.concatenate(
                    [a_ref[64 * x + 8 * at : 64 * x + 8 * at + 8, :] for x in range(8)], axis=0
                )
            else:
                layer = a_ref[pl.ds(at, 64, stride=8), :]
            first, second = layer[:32], layer[32:]
            faces_ref[12 * index + face] = jnp.where(low, first, pltpu.roll(second, 64, 1)).astype(BF16)
            faces_ref[12 * index + 6 + face] = jnp.where(low, pltpu.roll(first, 64, 1), second).astype(
                BF16
            )
        return carry

    lax.fori_loop(0, pairs, pair, 0)
    empty = 12 * pairs
    faces_ref[empty] = jnp.zeros((32, 128), BF16)

    for copy in copies[1:]:
        copy.wait()
    members, size = out_ref.shape[0], out_ref.shape[1] - 32 * slots
    place = lax.broadcasted_iota(jnp.int32, (size, 128), 0) * 128 + lax.broadcasted_iota(
        jnp.int32, (size, 128), 1
    )
    common = jnp.zeros((size, 128), jnp.int32)
    own_slots = [ref.shape[1] // members for ref in (sends1_ref, sends2_ref)]
    column, sent = 0, []
    for sends, parents, uplinks, count in (
        (sends1_ref, parents1_ref, uplinks1_ref, own_slots[0]),
        (sends2_ref, parents2_ref, uplinks2_ref, own_slots[1]),
    ):
        sent += [(column + k, sends, count, k) for k in range(count)]
        column += count
        for i in range(parents.shape[0] * 8):
            common = jnp.where(place == column, parents[i // 8, i % 8], common)
            column += 1
        for i in range(members):
            common = jnp.where(place == column, uplinks[0, i], common)
            column += 1

    def peer(index, carry):
        for slot in range(slots):
            row = sends_ref[0, slots * index + slot]
            out_ref[index, 32 * slot : 32 * slot + 32] = faces_ref[jnp.where(row < 0, empty, row)]
        table = common
        for at, sends, count, k in sent:
            table = jnp.where(place == at, sends[0, count * index + k], table)
        out_ref[index, 32 * slots : 32 * slots + size] = table.astype(F32).astype(BF16)
        return carry

    group = members // 4
    leaving = []
    for part in range(4):
        lax.fori_loop(part * group, (part + 1) * group, peer, 0)
        rows = pl.ds(part * group, group)
        leaving.append(pltpu.make_async_copy(out_ref.at[rows], out_hbm.at[rows], out_sems.at[part]))
        leaving[-1].start()
    leaving += fetch([(act_ref, act_hbm), (faces_ref, faces_hbm)], late_sems)
    for copy in leaving:
        copy.wait()


def inner_kernel(pairs, act_hbm, k_hbm, inner_ref, act_ref, k_ref, e_ref, lo_ref, hi_ref, p_ref, sems):
    copies = fetch([(act_hbm, act_ref), (k_hbm, k_ref)], sems)
    for ref in (e_ref, lo_ref, hi_ref):
        ref[...] = jnp.zeros_like(ref)
    for copy in copies:
        copy.wait()

    def pair(index, carry):
        for x in range(8):
            e_ref[80 * x + 88 : 80 * x + 152] = act_ref[index, 64 * x : 64 * x + 64].astype(F32)
        fill_columns(e_ref, lo_ref, hi_ref, p_ref)
        inner_ref[index] = contract(p_ref, k_ref)
        return carry

    lax.fori_loop(0, pairs, pair, 0)


def fine_kernel(
    pairs, links_ref, arrived_hbm, faces_hbm, inner_hbm, k_hbm, x_hbm, pool_hbm, out_ref, pooled_ref,
    arrived_ref, faces_ref, total_ref, k_ref, x_ref, pool_ref, s_ref, l_ref, r_ref, sems,
):
    copies = fetch(
        [
            (arrived_hbm, arrived_ref), (faces_hbm, faces_ref), (inner_hbm, total_ref), (k_hbm, k_ref),
            (x_hbm, x_ref), (pool_hbm, pool_ref),
        ],
        sems,
    )
    low = lax.broadcasted_iota(jnp.int32, (32, 128), 1) < 64
    own = 12 * pairs
    slots = arrived_ref.shape[1] // 32
    received = arrived_ref.shape[0] * slots
    copies[0].wait()
    copies[1].wait()

    def slab(row, start, count):
        there = (row >= own) & (row < own + received)
        place = jnp.clip(row - own, 0, received - 1)
        peer = divide(place, slots)
        first = pl.multiple_of((place - peer * slots) * 32, 32)
        mine = faces_ref[jnp.minimum(row, own), start : start + count].astype(F32)
        theirs = arrived_ref[peer, pl.ds(first + start, count), :].astype(F32)
        return jnp.where(there, theirs, mine)

    def row_of(direction, entry):
        at = full_rows(direction, entry)
        return jnp.broadcast_to(s_ref[at : at + 1], (8, 128))

    def group(direction, entry):
        at = full_rows(direction, entry)
        return s_ref[at : at + 8]

    def rims(index, carry):
        for way, direction in enumerate(DIRECTIONS):
            rows = [links_ref[2 * index + half, way] for half in range(2)]
            p = None if kind(direction) == 1 else fixed_at(direction)[0]
            if p != 7:
                count = 32 if p is None else 8
                first, second = [slab(row, 0, count) for row in rows]
                s_ref[64 * way : 64 * way + count] = jnp.where(low[:count], first, pltpu.roll(second, 64, 1))
            if p != 0:
                start = 0 if p is None else 24
                first, second = [slab(row, start, 32 - start) for row in rows]
                s_ref[64 * way + 32 + start : 64 * way + 64] = jnp.where(
                    low[start:], pltpu.roll(first, 64, 1), second
                )
        into = pl.multiple_of(index * 64, 64)

        def writer(side):
            def write(column, window):
                l_ref[side, pl.ds(into, 64), column * 128 : column * 128 + 128] = window

            return write

        zeros = jnp.zeros((8, 128), F32)
        for side, step in enumerate((-1, 1)):
            build_columns(
                [group((step, -1, 0), 0)]
                + [group((step, 0, 0), 8 * y) for y in range(8)]
                + [group((step, 1, 0), 0)],
                [row_of((step, -1, -1), 0)]
                + [row_of((step, 0, -1), y) for y in range(8)]
                + [row_of((step, 1, -1), 0)],
                [row_of((step, -1, 1), 0)]
                + [row_of((step, 0, 1), y) for y in range(8)]
                + [row_of((step, 1, 1), 0)],
                writer(side),
            )
            build_columns(
                [None] + [group((0, step, 0), 8 * x) for x in range(8)] + [None],
                [zeros] * 10,
                [zeros] * 10,
                writer(2 + side),
            )
            build_columns(
                [None] + [group((0, 0, step), 8 * x) for x in range(8)] + [None],
                [None] + [row_of((0, -1, step), x) for x in range(8)] + [None],
                [None] + [row_of((0, 1, step), x) for x in range(8)] + [None],
                writer(4 + side),
            )
        return carry

    lax.fori_loop(0, pairs, rims, 0)
    for copy in copies[2:]:
        copy.wait()
    for side in range(6):
        r_ref[side] = jnp.dot(l_ref[side], k_ref[side], preferred_element_type=F32)

    def finish(index, carry):
        def part(side, first, count):
            return r_ref[side, pl.ds(pl.multiple_of(index * 64 + first, 8), count), :]

        total_ref[index, 0:64] += part(0, 0, 64)
        total_ref[index, 448:512] += part(1, 0, 64)
        for x in range(8):
            total_ref[index, 64 * x : 64 * x + 8] += part(2, 8 * x, 8)
            total_ref[index, 64 * x + 56 : 64 * x + 64] += part(3, 8 * x, 8)
        for side, z in ((4, 0), (5, 7)):
            total_ref[index, pl.ds(z, 64, stride=8), :] += part(side, 0, 64)
        source = x_ref[pl.ds(2 * index, 2)].astype(F32).reshape(128, 512)
        result = (source + total_ref[index].T).astype(BF16)
        out_ref[pl.ds(2 * index, 2)] = result.reshape(2, 64, 512)
        pooled_ref[index] = lax.dot_general(
            pool_ref[...], result, (((1,), (1,)), ((), ())), preferred_element_type=F32
        ).astype(BF16)
        return carry

    lax.fori_loop(0, pairs, finish, 0)


def level_kernel(bricks, members, halves, pieces, pooled, *refs):
    index_refs, gain_ref, refs = refs[:4], refs[4], refs[5:]
    piece_refs, refs = refs[: len(pieces)], refs[len(pieces) :]
    k_ref, place_ref, sel_ref, lines_ref, points_ref, pool_ref, mask_ref, lift_ref = refs[:8]
    refs = refs[8:]
    out_ref, refs = refs[0], refs[1:]
    if pooled:
        pooled_ref, refs = refs[0], refs[1:]
    t_ref, x_ref, g_ref, s_ref, e_ref, lo_ref, hi_ref, p_ref = refs[:8]
    scalar_refs, sems = refs[8:12], refs[12]
    here_ref, links_ref, sends_ref, places_ref = scalar_refs
    work, at = list(zip(index_refs, scalar_refs)), 0
    for ref, size in zip(piece_refs, pieces):
        work.append((ref, t_ref.at[pl.ds(at, size)]))
        at += size
    copies = fetch(work, sems)
    t_ref[at] = jnp.zeros((64, 128), BF16)
    slots = sends_ref.shape[1]
    for copy in copies:
        copy.wait()
    me = here_ref[0, 0]

    def block(code):
        if halves == 1:
            return t_ref[code]
        return t_ref[lax.shift_right_logical(code, 1)] * mask_ref[code & 1]

    def activate(hidden):
        mean_sq = jnp.mean(hidden * hidden, axis=1, keepdims=True)
        return silu(hidden * lax.rsqrt(mean_sq + EPSILON) * gain_ref[...]).astype(BF16).astype(F32)

    def brick(index, carry):
        for octant in range(8):
            x_ref[64 * octant : 64 * octant + 64] = block(places_ref[8 * index + octant, me])
        grid = jnp.dot(place_ref[...], x_ref[...], preferred_element_type=F32).astype(BF16)
        hidden = jnp.dot(grid, lift_ref[...], preferred_element_type=F32).astype(BF16).astype(F32)
        active = activate(hidden)
        for x in range(8):
            e_ref[80 * x + 88 : 80 * x + 152] = active[64 * x : 64 * x + 64]
        for way, direction in enumerate(DIRECTIONS):
            row = links_ref[index, way]
            beyond = row - 6 * bricks
            inside = jnp.clip(beyond, 0, members * slots - 1)
            peer = divide(inside, slots)
            sent = sends_ref[peer, inside - peer * slots]
            device = jnp.where(beyond < 0, me, peer)
            row = jnp.where(beyond < 0, row, sent)
            usable = (row >= 0) & (beyond < members * slots)
            row = jnp.maximum(row, 0)
            source = lax.shift_right_logical(row * 43691, 18)
            face = row - 6 * source
            axis, side = lax.shift_right_logical(face, 1), 1 - (face & 1)

            def part(m):
                high, least = m // 2, m % 2
                octant = jnp.where(
                    axis == 0, 4 * side + m, jnp.where(axis == 1, 4 * high + 2 * side + least, 2 * m + side)
                )
                code = places_ref[8 * source + octant, device]
                return block(jnp.where(usable, code, at * halves))

            base = compact_base(direction)
            p, q = (None, None) if kind(direction) == 1 else fixed_at(direction)
            if kind(direction) == 1:
                tiles, weights, count = [part(m) for m in range(4)], sel_ref[face], 64
            elif kind(direction) == 2:
                if q is None:
                    tiles, variant = [part(2 * (p // 4)), part(2 * (p // 4) + 1)], 0 if p == 7 else 1
                else:
                    tiles, variant = [part(q // 4), part(2 + q // 4)], 2 if q == 7 else 3
                weights, count = lines_ref[4 * face + variant], 16
            else:
                tiles = [part(2 * (p // 4) + q // 4)]
                weights, count = points_ref[4 * face + (0 if p == 7 else 2) + (0 if q == 7 else 1)], 16
            g_ref[base : base + count] = jnp.dot(
                weights, jnp.concatenate(tiles, axis=0), preferred_element_type=F32
            ).astype(BF16)

        def lifted(step, carry):
            rows = pl.ds(pl.multiple_of(step * (COMPACT // 4), 16), COMPACT // 4)
            rim = jnp.dot(g_ref[rows, :], lift_ref[...], preferred_element_type=F32)
            s_ref[rows, :] = activate(rim.astype(BF16).astype(F32))
            return carry

        lax.fori_loop(0, 4, lifted, 0, unroll=True)
        fill_halo(s_ref, e_ref, lo_ref, hi_ref, compact_rows)
        fill_columns(e_ref, lo_ref, hi_ref, p_ref)

        result = (hidden + contract(p_ref, k_ref)).astype(BF16)
        out_ref[index] = result.astype(F32).T.astype(BF16)
        if pooled:
            pooled_ref[index] = jnp.dot(pool_ref[...], result, preferred_element_type=F32).astype(BF16)
        return carry

    lax.fori_loop(0, bricks, brick, 0)


def shift_pairs(size, step):
    half = size // 2
    return [(i, (i // 2 - step) % half * 2 + i % 2) for i in range(size)]


def flip_pairs(size):
    return [(i, i ^ 1) for i in range(size)]


def gather_blocks(blocks, nx, ny, beside):
    n = blocks.shape[0]
    half = n // 2
    column = [blocks] + [lax.ppermute(blocks, "gy", shift_pairs(ny, s)) for s in range(1, ny // 2)]
    first = jnp.concatenate([b[:half] for b in column], axis=0)
    second = jnp.concatenate([b[half:] for b in column], axis=0)
    if beside:
        first, second, *beside = lax.optimization_barrier((first, second, *beside))
    first = jnp.concatenate([first, lax.ppermute(first, "gy", flip_pairs(ny))], axis=0)
    second = jnp.concatenate(
        [second] + [lax.ppermute(second, "gx", shift_pairs(nx, s)) for s in range(1, nx // 2)], axis=0
    )
    here = [first] + [lax.ppermute(first, "gx", shift_pairs(nx, s)) for s in range(1, nx // 2)]
    here += [second, lax.ppermute(second, "gy", flip_pairs(ny))]
    return here + [lax.ppermute(b, "gx", flip_pairs(nx)) for b in here], beside


def block_place(device, local, n, nx, ny, mx, my):
    gx = divide(device, ny)
    gy = device - gx * ny
    half, columns, rows = n // 2, ny // 2, nx // 2
    core = (gx & 1) ^ (mx & 1)
    yi = modulo(divide(gx, 2) - divide(mx, 2) + rows, rows)
    xi = (gy & 1) ^ (my & 1)
    zi = modulo(divide(gy, 2) - divide(my, 2) + columns, columns)
    size = nx * ny // 2 * half
    first = ((yi * 2 + xi) * columns + zi) * half + local
    second = size + ((xi * rows + yi) * columns + zi) * half + local - half
    return core * 2 * size + jnp.where(local < half, first, second)


def places_kernel(nx, ny, levels, here_ref, table_ref, *refs):
    members = nx * ny
    mx, my = here_ref[0, 1], here_ref[0, 2]
    places_refs, sends_refs = refs[0::2], refs[1::2]
    column = 0
    for (bricks, slots, children, packed), places_ref, sends_ref in zip(levels, places_refs, sends_refs):
        parent_at, uplink_at = column + slots, column + slots + 8 * bricks
        sends_ref[...] = table_ref[:, column : column + slots]
        column = uplink_at + members
        tiles = children // packed
        parents = table_ref[:, parent_at : parent_at + 8 * bricks].astype(F32).T.astype(jnp.int32)
        uplinks = table_ref[:, uplink_at : uplink_at + members]
        child_of = lax.broadcasted_iota(jnp.int32, (members, members), 0)
        device = lax.broadcasted_iota(jnp.int32, (1, members), 1)
        for place in range(8 * bricks):
            row = parents[place : place + 1]
            peer = row - children
            owed = jnp.sum(jnp.where(child_of == peer, uplinks, 0), axis=0, keepdims=True)
            usable = (peer < 0) | ((peer < members) & (owed >= 0))
            source = jnp.where(peer < 0, device, jnp.clip(peer, 0, members - 1))
            local = jnp.maximum(jnp.where(peer < 0, row, owed), 0)
            where = block_place(source, divide(local, packed), tiles, nx, ny, mx, my)
            places_ref[place : place + 1] = jnp.where(
                usable, where * packed + modulo(local, packed), members * tiles * packed
            )


def run_level(here, links, sends, places, pieces, gain, lift, kernel, members, halves, pooled, consts):
    bricks, channels = links.shape[0], lift.shape[1]
    sizes = [piece.shape[0] for piece in pieces]
    held = [kernel, *consts, lift]
    outs = [jax.ShapeDtypeStruct((bricks, channels, 512), BF16)]
    if pooled:
        outs.append(jax.ShapeDtypeStruct((bricks, 64, channels), BF16))
    return pl.pallas_call(
        functools.partial(level_kernel, bricks, members, halves, sizes, pooled),
        out_shape=outs,
        in_specs=[ANY] * 4 + [VMEM] + [ANY] * len(pieces) + [VMEM] * len(held),
        out_specs=[VMEM] * len(outs),
        scratch_shapes=[
            pltpu.VMEM((sum(sizes) + 1, 64, 128), BF16),
            pltpu.VMEM((512, 128), BF16),
            pltpu.VMEM((COMPACT, 128), BF16),
            pltpu.VMEM((COMPACT, channels), F32),
            pltpu.VMEM((800, channels), F32),
            pltpu.VMEM((160, channels), F32),
            pltpu.VMEM((160, channels), F32),
            pltpu.VMEM((640, 9 * channels), BF16),
            *[pltpu.SMEM(value.shape, value.dtype) for value in (here, links, sends, places)],
            pltpu.SemaphoreType.DMA((4 + len(pieces),)),
        ],
        compiler_params=grant(sum(sizes) * 33_000 + channels * 90_000),
        name="level" + str(channels),
    )(here, links, sends, places, gain[None, :], *pieces, *held)


def per_device(
    nx, ny,
    voxels_fine, gain_fine, gain_middle, gain_coarse, kernel_fine, kernel_middle, kernel_coarse,
    lift_middle, lift_coarse, links_fine, links_middle, links_coarse, sends_fine, sends_middle,
    sends_coarse, parents_middle, parents_coarse, uplinks_middle, uplinks_coarse,
):
    members = nx * ny
    bricks0, bricks1, bricks2 = voxels_fine.shape[0], links_middle.shape[0], links_coarse.shape[0]
    pairs = bricks0 // 2
    pool = pool_matrix()

    mx, my = lax.axis_index("gx"), lax.axis_index("gy")
    here = jnp.stack([mx * ny + my, mx, my])[None].astype(jnp.int32)
    assert members + bricks0 <= 256 and 6 * bricks1 <= 256
    width = sum(
        table.shape[-1]
        for table in (sends_middle.reshape(members, -1), sends_coarse.reshape(members, -1), uplinks_middle, uplinks_coarse)
    ) + 8 * (bricks1 + bricks2)
    size = -(-width // 1024) * 8
    slots = sends_fine.shape[1] // members

    indices = (
        sends_fine, sends_middle, sends_coarse, parents_middle, parents_coarse, uplinks_middle, uplinks_coarse,
    )
    act, faces, outgoing = pl.pallas_call(
        functools.partial(pack_kernel, pairs, slots),
        out_shape=[
            jax.ShapeDtypeStruct((pairs, 512, 128), BF16),
            jax.ShapeDtypeStruct((12 * pairs + 1, 32, 128), BF16),
            jax.ShapeDtypeStruct((members, 32 * slots + size, 128), BF16),
        ],
        in_specs=[ANY] * 7 + [ANY, VMEM],
        out_specs=[HBM] * 3,
        scratch_shapes=[
            *[pltpu.SMEM(value.shape, value.dtype) for value in indices],
            pltpu.VMEM(voxels_fine.shape, BF16),
            pltpu.VMEM((pairs, 512, 128), BF16),
            pltpu.VMEM((12 * pairs + 1, 32, 128), BF16),
            pltpu.VMEM((members, 32 * slots + size, 128), BF16),
            pltpu.VMEM((512, 128), F32),
            pltpu.SemaphoreType.DMA((8,)),
            pltpu.SemaphoreType.DMA((4,)),
            pltpu.SemaphoreType.DMA((2,)),
        ],
        compiler_params=grant(WHOLE),
        name="pack",
    )(*indices, voxels_fine, gain_fine[None])

    outgoing, act, kernel_fine, kernel_middle, kernel_coarse = lax.optimization_barrier(
        (outgoing, act, kernel_fine, kernel_middle, kernel_coarse)
    )
    arrived = lax.all_to_all(outgoing, AXES, split_axis=0, concat_axis=0, tiled=True)

    slots1, slots2 = sends_middle.shape[1] // members, sends_coarse.shape[1] // members
    levels = ((bricks1, slots1, bricks0, 2), (bricks2, slots2, bricks1, 1))
    def columns(kernel):
        return kernel.transpose(0, 2, 1).reshape(3, 9 * kernel.shape[2], kernel.shape[1])

    def side_by_side(kernel):
        first = jnp.concatenate([kernel[0], kernel[1]], axis=1)
        return jnp.stack([first, jnp.concatenate([kernel[2], jnp.zeros_like(kernel[2])], axis=1)])

    turned = kernel_fine.transpose(0, 2, 1)
    blank = jnp.zeros_like(turned)
    kernel0 = jnp.concatenate(
        [jnp.concatenate([turned, blank], axis=2), jnp.concatenate([blank, turned], axis=2)], axis=1
    ).reshape(3, 9 * 128, 128)
    kernel1, kernel2 = columns(kernel_middle), columns(kernel_coarse)
    kernel1 = side_by_side(kernel1)
    lift1 = jnp.concatenate([lift_middle.T, lift_middle.T], axis=0)
    lift2 = lift_coarse.T
    cube = kernel0.reshape(3, 3, 3, 128, 128)
    rim0 = jnp.stack(
        [part.reshape(9 * 128, 128) for at in ((0,), (slice(None), 0), (slice(None), slice(None), 0))
         for part in (cube[at], cube[at[:-1] + (2,)])]
    )
    inner = pl.pallas_call(
        functools.partial(inner_kernel, pairs),
        out_shape=jax.ShapeDtypeStruct((pairs, 512, 128), F32),
        in_specs=[HBM] * 2,
        out_specs=VMEM,
        scratch_shapes=[
            pltpu.VMEM(act.shape, BF16),
            pltpu.VMEM((2, 9 * 128, 256), BF16),
            pltpu.VMEM((800, 128), F32),
            pltpu.VMEM((160, 128), F32),
            pltpu.VMEM((160, 128), F32),
            pltpu.VMEM((640, 9 * 128), BF16),
            pltpu.SemaphoreType.DMA((2,)),
        ],
        compiler_params=grant(WHOLE),
        name="inner",
    )(act, side_by_side(kernel0))
    arrived, inner, rim0, kernel1, kernel2, lift1, lift2 = lax.optimization_barrier(
        (arrived, inner, rim0, kernel1, kernel2, lift1, lift2)
    )

    output_fine, pooled_fine = pl.pallas_call(
        functools.partial(fine_kernel, pairs),
        out_shape=[
            jax.ShapeDtypeStruct(voxels_fine.shape, BF16),
            jax.ShapeDtypeStruct((pairs, 64, 128), BF16),
        ],
        in_specs=[SMEM] + [HBM] * 6,
        out_specs=[VMEM] * 2,
        scratch_shapes=[
            *[pltpu.VMEM(value.shape, value.dtype) for value in (arrived, faces, inner, rim0, voxels_fine, pool)],
            pltpu.VMEM((64 * WAYS, 128), F32),
            pltpu.VMEM((6, 64 * pairs, 9 * 128), BF16),
            pltpu.VMEM((6, 64 * pairs, 128), F32),
            pltpu.SemaphoreType.DMA((6,)),
        ],
        compiler_params=grant(WHOLE),
        name="fine",
    )(links_fine, arrived, faces, inner, rim0, voxels_fine, pool)

    consts = (place_matrix(), face_matrices(), *rim_matrices(), pool, half_masks())
    table = arrived[:, 32 * slots :].reshape(members, -1)[:, :width].astype(F32).astype(jnp.int32)
    places1, here1, places2, here2 = pl.pallas_call(
        functools.partial(places_kernel, nx, ny, levels),
        out_shape=[
            jax.ShapeDtypeStruct(shape, jnp.int32)
            for bricks, slots_, _, _ in levels
            for shape in ((8 * bricks, members), (members, slots_))
        ],
        in_specs=[SMEM, VMEM],
        out_specs=[VMEM] * 4,
        compiler_params=grant(4_000_000),
        name="places",
    )(here, table)
    blocks, (places1, here1, places2, here2) = gather_blocks(
        pooled_fine, nx, ny, (places1, here1, places2, here2)
    )
    output_middle, pooled_middle = run_level(
        here, links_middle, here1, places1, blocks, gain_middle, lift1, kernel1,
        members, 2, True, consts,
    )
    (output_coarse,) = run_level(
        here, links_coarse, here2, places2, gather_blocks(pooled_middle, nx, ny, ())[0], gain_coarse, lift2, kernel2,
        members, 1, False, consts,
    )
    return (output_fine, output_middle, output_coarse)


def solution(mesh):
    nx, ny = mesh.shape["gx"], mesh.shape["gy"]
    split3, split2, whole = P(AXES, None, None), P(AXES, None), P()
    return jax.shard_map(
        functools.partial(per_device, nx, ny),
        mesh=mesh,
        in_specs=(split3,) + (whole,) * 8 + (split2,) * 10,
        out_specs=(split3,) * 3,
        check_vma=False,
    )
```

```python
import functools
import jax
import jax.numpy as jnp
import numpy as np
from jax import lax
from jax.experimental import pallas as pl
from jax.experimental.pallas import tpu as pltpu
from jax.sharding import PartitionSpec as P

EPSILON = 1e-06
AXES = ("gx", "gy")
DIRECTIONS = [
    (a, b, c) for a in (-1, 0, 1) for b in (-1, 0, 1) for c in (-1, 0, 1) if (a, b, c) != (0, 0, 0)
]
DIR = {direction: place for place, direction in enumerate(DIRECTIONS)}
WAYS = len(DIRECTIONS)
VMEM = pl.BlockSpec(memory_space=pltpu.VMEM)
SMEM = pl.BlockSpec(memory_space=pltpu.SMEM)
ANY = pl.BlockSpec(memory_space=pl.ANY)
HBM = pl.BlockSpec(memory_space=pltpu.HBM)
F32 = jnp.float32
BF16 = jnp.bfloat16


def pool_matrix():
    matrix = np.zeros((64, 512), np.float32)
    for x in range(8):
        for y in range(8):
            for z in range(8):
                matrix[(x // 2) * 16 + (y // 2) * 4 + z // 2, x * 64 + y * 8 + z] = 0.125
    return jnp.asarray(matrix, BF16)


def place_matrix():
    matrix = np.zeros((512, 512), np.float32)
    for x in range(8):
        for y in range(8):
            for z in range(8):
                octant = (x // 4) * 4 + (y // 4) * 2 + z // 4
                inner = (x % 4) * 16 + (y % 4) * 4 + z % 4
                matrix[x * 64 + y * 8 + z, octant * 64 + inner] = 1
    return jnp.asarray(matrix, BF16)


def face_matrices():
    matrices = np.zeros((6, 64, 256), np.float32)
    for face in range(6):
        axis, layer = face // 2, 3 if face % 2 == 0 else 0
        for p in range(8):
            for q in range(8):
                inner = [p % 4, q % 4]
                inner.insert(axis, layer)
                octant = (p // 4) * 2 + q // 4
                matrices[face, p * 8 + q, octant * 64 + inner[0] * 16 + inner[1] * 4 + inner[2]] = 1
    return jnp.asarray(matrices, BF16)


def rim_matrices():
    lines = np.zeros((6, 4, 16, 128), np.float32)
    points = np.zeros((6, 4, 16, 64), np.float32)
    for face in range(6):
        axis, layer = face // 2, 3 if face % 2 == 0 else 0

        def inner(p, q):
            cell = [p % 4, q % 4]
            cell.insert(axis, layer)
            return cell[0] * 16 + cell[1] * 4 + cell[2]

        for side, fixed in enumerate((7, 0)):
            for e in range(8):
                lines[face, side, e, (e // 4) * 64 + inner(fixed, e)] = 1
                lines[face, 2 + side, e, (e // 4) * 64 + inner(e, fixed)] = 1
            for other, second in enumerate((7, 0)):
                points[face, 2 * side + other, 0, inner(fixed, second)] = 1
    return jnp.asarray(lines.reshape(24, 16, 128), BF16), jnp.asarray(points.reshape(24, 16, 64), BF16)


def half_masks():
    masks = np.zeros((2, 64, 128), np.float32)
    masks[0, :, :64] = 1
    masks[1, :, 64:] = 1
    return jnp.asarray(masks, BF16)


WHOLE = 65_500_000


def grant(size):
    return pltpu.CompilerParams(vmem_limit_bytes=min(size, WHOLE))


def divide(value, by):
    return lax.shift_right_arithmetic(value, by.bit_length() - 1) if by & (by - 1) == 0 else value // by


def modulo(value, by):
    return value & (by - 1) if by & (by - 1) == 0 else lax.rem(value, by)


def fetch(pairs, sems):
    copies = [pltpu.make_async_copy(src, dst, sems.at[i]) for i, (src, dst) in enumerate(pairs)]
    for copy in copies:
        copy.start()
    return copies


def silu(v):
    return v / (1.0 + jnp.exp(-v))


def kind(direction):
    return sum(1 for step in direction if step != 0)


def fixed_at(direction):
    leading = next(axis for axis in range(3) if direction[axis] != 0)
    rest = [direction[axis] for axis in range(3) if axis != leading]
    return [None if step == 0 else 7 if step < 0 else 0 for step in rest]


def full_rows(direction, entry):
    base = DIR[direction] * 64
    if kind(direction) == 1:
        return base + entry
    p, q = fixed_at(direction)
    if kind(direction) == 3:
        return base + 8 * p + q
    return base + (8 * p + entry if q is None else 8 * entry + q)


FACES = [d for d in DIRECTIONS if kind(d) == 1]
EDGES = [d for d in DIRECTIONS if kind(d) == 2]
CORNERS = [d for d in DIRECTIONS if kind(d) == 3]
COMPACT = 64 * len(FACES) + 16 * len(EDGES) + 16 * len(CORNERS)


def compact_base(direction):
    if kind(direction) == 1:
        return 64 * FACES.index(direction)
    if kind(direction) == 2:
        return 64 * len(FACES) + 16 * EDGES.index(direction)
    return 64 * len(FACES) + 16 * len(EDGES) + 16 * CORNERS.index(direction)


def compact_rows(direction, entry):
    return compact_base(direction) + entry


def fill_halo(s_ref, e_ref, lo_ref, hi_ref, rows):
    def take(ref, at, direction, first, count):
        source = rows(direction, first)
        if rows(direction, first + count - 1) == source + count - 1:
            ref[at : at + count] = s_ref[source : source + count]
        else:
            ref[at : at + count] = s_ref[pl.ds(source, count, stride=8), :]

    for a, plane in ((-1, 0), (1, 9)):
        base, rim = plane * 80, plane * 16
        take(e_ref, base + 8, (a, 0, 0), 0, 64)
        take(e_ref, base, (a, -1, 0), 0, 8)
        take(e_ref, base + 72, (a, 1, 0), 0, 8)
        for ref, c in ((lo_ref, -1), (hi_ref, 1)):
            take(ref, rim, (a, 0, c), 0, 8)
            take(ref, rim + 8, (a, -1, c), 0, 1)
            take(ref, rim + 9, (a, 1, c), 0, 1)
    for x in range(8):
        base, rim = (x + 1) * 80, (x + 1) * 16
        take(e_ref, base, (0, -1, 0), 8 * x, 8)
        take(e_ref, base + 72, (0, 1, 0), 8 * x, 8)
        for ref, c in ((lo_ref, -1), (hi_ref, 1)):
            take(ref, rim, (0, 0, c), 8 * x, 8)
            take(ref, rim + 8, (0, -1, c), x, 1)
            take(ref, rim + 9, (0, 1, c), x, 1)


def build_columns(middles, lows, highs, write):
    within = lax.broadcasted_iota(jnp.int32, middles[1].shape, 0)
    shifted = ([], [], [])
    for middle, low, high in zip(middles, lows, highs):
        if middle is None:
            middle = jnp.zeros_like(middles[1])
            for variant in shifted:
                variant.append(middle)
            continue
        before, after = pltpu.roll(middle, 1, 0), pltpu.roll(middle, 7, 0)
        shifted[0].append(jnp.where(within == 0, low, before))
        shifted[1].append(middle)
        shifted[2].append(jnp.where(within == 7, high, after))
    for d in range(3):
        for e in range(3):
            write(3 * d + e, jnp.concatenate(shifted[e][d : d + 8], axis=0).astype(BF16))


def fill_columns(e_ref, lo_ref, hi_ref, p_ref):
    channels = e_ref.shape[1]

    def plane(index, carry):
        base = pl.multiple_of(index * 80, 8)
        rim = pl.multiple_of(index * 16, 8)
        into = pl.multiple_of(index * 64, 64)

        def edge(ref, y):
            at = 8 if y == 0 else 9 if y == 9 else y - 1
            return jnp.broadcast_to(ref[pl.ds(rim + at, 1), :], (8, channels))

        def write(column, window):
            p_ref[pl.ds(into, 64), column * channels : (column + 1) * channels] = window

        build_columns(
            [e_ref[pl.ds(base + 8 * y, 8), :] for y in range(10)],
            [edge(lo_ref, y) for y in range(10)],
            [edge(hi_ref, y) for y in range(10)],
            write,
        )
        return carry

    lax.fori_loop(0, 10, plane, 0)


def contract(p_ref, k_ref):
    channels = k_ref.shape[2]
    if k_ref.shape[0] == 3:
        rows = jnp.concatenate([p_ref[64 * dx : 64 * dx + 512, :] for dx in range(3)], axis=1)
        return jnp.dot(rows, k_ref[...].reshape(-1, channels), preferred_element_type=F32)
    both = jnp.dot(p_ref[0:576, :], k_ref[0], preferred_element_type=F32)
    last = jnp.dot(p_ref[128:640, :], k_ref[1][:, :128], preferred_element_type=F32)
    return both[0:512, :128] + both[64:576, 128:] + last


def pack_kernel(
    pairs, slots, *refs,
):
    index_hbm, (x_hbm, gain_ref, act_hbm, faces_hbm, out_hbm), refs = refs[:7], refs[7:12], refs[12:]
    index_refs, (x_ref, act_ref, faces_ref, out_ref, a_ref, sems, out_sems, late_sems) = refs[:7], refs[7:]
    sends_ref, sends1_ref, sends2_ref, parents1_ref, parents2_ref, uplinks1_ref, uplinks2_ref = index_refs
    copies = fetch([(x_hbm, x_ref), *zip(index_hbm, index_refs)], sems)
    low = lax.broadcasted_iota(jnp.int32, (32, 128), 1) < 64
    gain = jnp.broadcast_to(gain_ref[...], (128, 64)).T[:, :1][None]
    copies[0].wait()

    def pair(index, carry):
        values = x_ref[pl.ds(2 * index, 2)].astype(F32)
        mean_sq = jnp.mean(values * values, axis=1, keepdims=True)
        scaled = values * lax.rsqrt(mean_sq + EPSILON) * gain
        rounded = silu(scaled).astype(BF16).astype(F32).reshape(128, 512)
        a_ref[...] = rounded.T
        act_ref[index] = a_ref[...].astype(BF16)
        for face in range(6):
            axis, at = face // 2, 7 if face % 2 == 0 else 0
            if axis == 0:
                layer = a_ref[64 * at : 64 * at + 64, :]
            elif axis == 1:
                layer = jnp.concatenate(
                    [a_ref[64 * x + 8 * at : 64 * x + 8 * at + 8, :] for x in range(8)], axis=0
                )
            else:
                layer = a_ref[pl.ds(at, 64, stride=8), :]
            first, second = layer[:32], layer[32:]
            faces_ref[12 * index + face] = jnp.where(low, first, pltpu.roll(second, 64, 1)).astype(BF16)
            faces_ref[12 * index + 6 + face] = jnp.where(low, pltpu.roll(first, 64, 1), second).astype(
                BF16
            )
        return carry

    lax.fori_loop(0, pairs, pair, 0)
    empty = 12 * pairs
    faces_ref[empty] = jnp.zeros((32, 128), BF16)

    for copy in copies[1:]:
        copy.wait()
    members, size = out_ref.shape[0], out_ref.shape[1] - 32 * slots
    place = lax.broadcasted_iota(jnp.int32, (size, 128), 0) * 128 + lax.broadcasted_iota(
        jnp.int32, (size, 128), 1
    )
    common = jnp.zeros((size, 128), jnp.int32)
    own_slots = [ref.shape[1] // members for ref in (sends1_ref, sends2_ref)]
    column, sent = 0, []
    for sends, parents, uplinks, count in (
        (sends1_ref, parents1_ref, uplinks1_ref, own_slots[0]),
        (sends2_ref, parents2_ref, uplinks2_ref, own_slots[1]),
    ):
        sent += [(column + k, sends, count, k) for k in range(count)]
        column += count
        for i in range(parents.shape[0] * 8):
            common = jnp.where(place == column, parents[i // 8, i % 8], common)
            column += 1
        for i in range(members):
            common = jnp.where(place == column, uplinks[0, i], common)
            column += 1

    def peer(index, carry):
        for slot in range(slots):
            row = sends_ref[0, slots * index + slot]
            out_ref[index, 32 * slot : 32 * slot + 32] = faces_ref[jnp.where(row < 0, empty, row)]
        table = common
        for at, sends, count, k in sent:
            table = jnp.where(place == at, sends[0, count * index + k], table)
        out_ref[index, 32 * slots : 32 * slots + size] = table.astype(F32).astype(BF16)
        return carry

    group = members // 4
    leaving = []
    for part in range(4):
        lax.fori_loop(part * group, (part + 1) * group, peer, 0)
        rows = pl.ds(part * group, group)
        leaving.append(pltpu.make_async_copy(out_ref.at[rows], out_hbm.at[rows], out_sems.at[part]))
        leaving[-1].start()
    leaving += fetch([(act_ref, act_hbm), (faces_ref, faces_hbm)], late_sems)
    for copy in leaving:
        copy.wait()


def inner_kernel(pairs, act_hbm, k_hbm, inner_ref, act_ref, k_ref, e_ref, lo_ref, hi_ref, p_ref, sems):
    copies = fetch([(act_hbm, act_ref), (k_hbm, k_ref)], sems)
    for ref in (e_ref, lo_ref, hi_ref):
        ref[...] = jnp.zeros_like(ref)
    for copy in copies:
        copy.wait()

    def pair(index, carry):
        for x in range(8):
            e_ref[80 * x + 88 : 80 * x + 152] = act_ref[index, 64 * x : 64 * x + 64].astype(F32)
        fill_columns(e_ref, lo_ref, hi_ref, p_ref)
        inner_ref[index] = contract(p_ref, k_ref)
        return carry

    lax.fori_loop(0, pairs, pair, 0)


def fine_kernel(
    pairs, links_any, arrived_hbm, faces_hbm, inner_hbm, k_hbm, x_hbm, pool_hbm, out_ref, pooled_ref,
    links_ref, arrived_ref, faces_ref, total_ref, k_ref, x_ref, pool_ref, s_ref, l_ref, r_ref, sems,
):
    copies = fetch(
        [
            (links_any, links_ref), (arrived_hbm, arrived_ref), (faces_hbm, faces_ref), (inner_hbm, total_ref),
            (k_hbm, k_ref), (x_hbm, x_ref), (pool_hbm, pool_ref),
        ],
        sems,
    )
    low = lax.broadcasted_iota(jnp.int32, (32, 128), 1) < 64
    own = 12 * pairs
    slots = arrived_ref.shape[1] // 32
    received = arrived_ref.shape[0] * slots
    for copy in copies[:3]:
        copy.wait()

    def slab(row, start, count):
        there = (row >= own) & (row < own + received)
        place = jnp.clip(row - own, 0, received - 1)
        peer = divide(place, slots)
        first = pl.multiple_of((place - peer * slots) * 32, 32)
        mine = faces_ref[jnp.minimum(row, own), start : start + count].astype(F32)
        theirs = arrived_ref[peer, pl.ds(first + start, count), :].astype(F32)
        return jnp.where(there, theirs, mine)

    def row_of(direction, entry):
        at = full_rows(direction, entry)
        return jnp.broadcast_to(s_ref[at : at + 1], (8, 128))

    def group(direction, entry):
        at = full_rows(direction, entry)
        return s_ref[at : at + 8]

    def rims(index, carry):
        for way, direction in enumerate(DIRECTIONS):
            rows = [links_ref[2 * index + half, way] for half in range(2)]
            p = None if kind(direction) == 1 else fixed_at(direction)[0]
            if p != 7:
                count = 32 if p is None else 8
                first, second = [slab(row, 0, count) for row in rows]
                s_ref[64 * way : 64 * way + count] = jnp.where(low[:count], first, pltpu.roll(second, 64, 1))
            if p != 0:
                start = 0 if p is None else 24
                first, second = [slab(row, start, 32 - start) for row in rows]
                s_ref[64 * way + 32 + start : 64 * way + 64] = jnp.where(
                    low[start:], pltpu.roll(first, 64, 1), second
                )
        into = pl.multiple_of(index * 64, 64)

        def writer(side):
            def write(column, window):
                l_ref[side, pl.ds(into, 64), column * 128 : column * 128 + 128] = window

            return write

        zeros = jnp.zeros((8, 128), F32)
        for side, step in enumerate((-1, 1)):
            build_columns(
                [group((step, -1, 0), 0)]
                + [group((step, 0, 0), 8 * y) for y in range(8)]
                + [group((step, 1, 0), 0)],
                [row_of((step, -1, -1), 0)]
                + [row_of((step, 0, -1), y) for y in range(8)]
                + [row_of((step, 1, -1), 0)],
                [row_of((step, -1, 1), 0)]
                + [row_of((step, 0, 1), y) for y in range(8)]
                + [row_of((step, 1, 1), 0)],
                writer(side),
            )
            build_columns(
                [None] + [group((0, step, 0), 8 * x) for x in range(8)] + [None],
                [zeros] * 10,
                [zeros] * 10,
                writer(2 + side),
            )
            build_columns(
                [None] + [group((0, 0, step), 8 * x) for x in range(8)] + [None],
                [None] + [row_of((0, -1, step), x) for x in range(8)] + [None],
                [None] + [row_of((0, 1, step), x) for x in range(8)] + [None],
                writer(4 + side),
            )
        return carry

    lax.fori_loop(0, pairs, rims, 0)
    for copy in copies[3:]:
        copy.wait()
    for side in range(6):
        r_ref[side] = jnp.dot(l_ref[side], k_ref[side], preferred_element_type=F32)

    def finish(index, carry):
        def part(side, first, count):
            return r_ref[side, pl.ds(pl.multiple_of(index * 64 + first, 8), count), :]

        total_ref[index, 0:64] += part(0, 0, 64)
        total_ref[index, 448:512] += part(1, 0, 64)
        for x in range(8):
            total_ref[index, 64 * x : 64 * x + 8] += part(2, 8 * x, 8)
            total_ref[index, 64 * x + 56 : 64 * x + 64] += part(3, 8 * x, 8)
        for side, z in ((4, 0), (5, 7)):
            total_ref[index, pl.ds(z, 64, stride=8), :] += part(side, 0, 64)
        source = x_ref[pl.ds(2 * index, 2)].astype(F32).reshape(128, 512)
        result = (source + total_ref[index].T).astype(BF16)
        out_ref[pl.ds(2 * index, 2)] = result.reshape(2, 64, 512)
        pooled_ref[index] = lax.dot_general(
            pool_ref[...], result, (((1,), (1,)), ((), ())), preferred_element_type=F32
        ).astype(BF16)
        return carry

    lax.fori_loop(0, pairs, finish, 0)


def level_kernel(bricks, members, halves, pieces, pooled, *refs):
    index_refs, gain_ref, refs = refs[:4], refs[4], refs[5:]
    piece_refs, refs = refs[: len(pieces)], refs[len(pieces) :]
    k_ref, place_ref, sel_ref, lines_ref, points_ref, pool_ref, mask_ref, lift_ref = refs[:8]
    refs = refs[8:]
    out_ref, refs = refs[0], refs[1:]
    if pooled:
        pooled_ref, refs = refs[0], refs[1:]
    t_ref, x_ref, g_ref, s_ref, e_ref, lo_ref, hi_ref, p_ref = refs[:8]
    scalar_refs, sems = refs[8:12], refs[12]
    here_ref, links_ref, sends_ref, places_ref = scalar_refs
    work, at = list(zip(index_refs, scalar_refs)), 0
    for ref, size in zip(piece_refs, pieces):
        work.append((ref, t_ref.at[pl.ds(at, size)]))
        at += size
    copies = fetch(work, sems)
    t_ref[at] = jnp.zeros((64, 128), BF16)
    slots = sends_ref.shape[1]
    for copy in copies:
        copy.wait()
    me = here_ref[0, 0]

    def block(code):
        if halves == 1:
            return t_ref[code]
        return t_ref[lax.shift_right_logical(code, 1)] * mask_ref[code & 1]

    def activate(hidden):
        mean_sq = jnp.mean(hidden * hidden, axis=1, keepdims=True)
        return silu(hidden * lax.rsqrt(mean_sq + EPSILON) * gain_ref[...]).astype(BF16).astype(F32)

    def brick(index, carry):
        for octant in range(8):
            x_ref[64 * octant : 64 * octant + 64] = block(places_ref[8 * index + octant, me])
        grid = jnp.dot(place_ref[...], x_ref[...], preferred_element_type=F32).astype(BF16)
        hidden = jnp.dot(grid, lift_ref[...], preferred_element_type=F32).astype(BF16).astype(F32)
        active = activate(hidden)
        for x in range(8):
            e_ref[80 * x + 88 : 80 * x + 152] = active[64 * x : 64 * x + 64]
        for way, direction in enumerate(DIRECTIONS):
            row = links_ref[index, way]
            beyond = row - 6 * bricks
            inside = jnp.clip(beyond, 0, members * slots - 1)
            peer = divide(inside, slots)
            sent = sends_ref[peer, inside - peer * slots]
            device = jnp.where(beyond < 0, me, peer)
            row = jnp.where(beyond < 0, row, sent)
            usable = (row >= 0) & (beyond < members * slots)
            row = jnp.maximum(row, 0)
            source = lax.shift_right_logical(row * 43691, 18)
            face = row - 6 * source
            axis, side = lax.shift_right_logical(face, 1), 1 - (face & 1)

            def part(m):
                high, least = m // 2, m % 2
                octant = jnp.where(
                    axis == 0, 4 * side + m, jnp.where(axis == 1, 4 * high + 2 * side + least, 2 * m + side)
                )
                code = places_ref[8 * source + octant, device]
                return block(jnp.where(usable, code, at * halves))

            base = compact_base(direction)
            p, q = (None, None) if kind(direction) == 1 else fixed_at(direction)
            if kind(direction) == 1:
                tiles, weights, count = [part(m) for m in range(4)], sel_ref[face], 64
            elif kind(direction) == 2:
                if q is None:
                    tiles, variant = [part(2 * (p // 4)), part(2 * (p // 4) + 1)], 0 if p == 7 else 1
                else:
                    tiles, variant = [part(q // 4), part(2 + q // 4)], 2 if q == 7 else 3
                weights, count = lines_ref[4 * face + variant], 16
            else:
                tiles = [part(2 * (p // 4) + q // 4)]
                weights, count = points_ref[4 * face + (0 if p == 7 else 2) + (0 if q == 7 else 1)], 16
            g_ref[base : base + count] = jnp.dot(
                weights, jnp.concatenate(tiles, axis=0), preferred_element_type=F32
            ).astype(BF16)

        def lifted(step, carry):
            rows = pl.ds(pl.multiple_of(step * (COMPACT // 4), 16), COMPACT // 4)
            rim = jnp.dot(g_ref[rows, :], lift_ref[...], preferred_element_type=F32)
            s_ref[rows, :] = activate(rim.astype(BF16).astype(F32))
            return carry

        lax.fori_loop(0, 4, lifted, 0, unroll=True)
        fill_halo(s_ref, e_ref, lo_ref, hi_ref, compact_rows)
        fill_columns(e_ref, lo_ref, hi_ref, p_ref)

        result = (hidden + contract(p_ref, k_ref)).astype(BF16)
        out_ref[index] = result.astype(F32).T.astype(BF16)
        if pooled:
            pooled_ref[index] = jnp.dot(pool_ref[...], result, preferred_element_type=F32).astype(BF16)
        return carry

    lax.fori_loop(0, bricks, brick, 0)


def shift_pairs(size, step):
    half = size // 2
    return [(i, (i // 2 - step) % half * 2 + i % 2) for i in range(size)]


def flip_pairs(size):
    return [(i, i ^ 1) for i in range(size)]


def gather_blocks(blocks, nx, ny, beside):
    n = blocks.shape[0]
    half = n // 2
    column = [blocks] + [lax.ppermute(blocks, "gy", shift_pairs(ny, s)) for s in range(1, ny // 2)]
    first = jnp.concatenate([b[:half] for b in column], axis=0)
    second = jnp.concatenate([b[half:] for b in column], axis=0)
    if beside:
        first, second, *beside = lax.optimization_barrier((first, second, *beside))
    first = jnp.concatenate([first, lax.ppermute(first, "gy", flip_pairs(ny))], axis=0)
    second = jnp.concatenate(
        [second] + [lax.ppermute(second, "gx", shift_pairs(nx, s)) for s in range(1, nx // 2)], axis=0
    )
    here = [first] + [lax.ppermute(first, "gx", shift_pairs(nx, s)) for s in range(1, nx // 2)]
    here += [second, lax.ppermute(second, "gy", flip_pairs(ny))]
    return here + [lax.ppermute(b, "gx", flip_pairs(nx)) for b in here], beside


def block_place(device, local, n, nx, ny, mx, my):
    gx = divide(device, ny)
    gy = device - gx * ny
    half, columns, rows = n // 2, ny // 2, nx // 2
    core = (gx & 1) ^ (mx & 1)
    yi = modulo(divide(gx, 2) - divide(mx, 2) + rows, rows)
    xi = (gy & 1) ^ (my & 1)
    zi = modulo(divide(gy, 2) - divide(my, 2) + columns, columns)
    size = nx * ny // 2 * half
    first = ((yi * 2 + xi) * columns + zi) * half + local
    second = size + ((xi * rows + yi) * columns + zi) * half + local - half
    return core * 2 * size + jnp.where(local < half, first, second)


def places_kernel(nx, ny, levels, here_ref, table_ref, *refs):
    members = nx * ny
    mx, my = here_ref[0, 1], here_ref[0, 2]
    places_refs, sends_refs = refs[0::2], refs[1::2]
    column = 0
    for (bricks, slots, children, packed), places_ref, sends_ref in zip(levels, places_refs, sends_refs):
        parent_at, uplink_at = column + slots, column + slots + 8 * bricks
        sends_ref[...] = table_ref[:, column : column + slots]
        column = uplink_at + members
        tiles = children // packed
        parents = table_ref[:, parent_at : parent_at + 8 * bricks].astype(F32).T.astype(jnp.int32)
        uplinks = table_ref[:, uplink_at : uplink_at + members]
        child_of = lax.broadcasted_iota(jnp.int32, (members, members), 0)
        device = lax.broadcasted_iota(jnp.int32, (1, members), 1)
        for place in range(8 * bricks):
            row = parents[place : place + 1]
            peer = row - children
            owed = jnp.sum(jnp.where(child_of == peer, uplinks, 0), axis=0, keepdims=True)
            usable = (peer < 0) | ((peer < members) & (owed >= 0))
            source = jnp.where(peer < 0, device, jnp.clip(peer, 0, members - 1))
            local = jnp.maximum(jnp.where(peer < 0, row, owed), 0)
            where = block_place(source, divide(local, packed), tiles, nx, ny, mx, my)
            places_ref[place : place + 1] = jnp.where(
                usable, where * packed + modulo(local, packed), members * tiles * packed
            )


def run_level(here, links, sends, places, pieces, gain, lift, kernel, members, halves, pooled, consts):
    bricks, channels = links.shape[0], lift.shape[1]
    sizes = [piece.shape[0] for piece in pieces]
    held = [kernel, *consts, lift]
    outs = [jax.ShapeDtypeStruct((bricks, channels, 512), BF16)]
    if pooled:
        outs.append(jax.ShapeDtypeStruct((bricks, 64, channels), BF16))
    return pl.pallas_call(
        functools.partial(level_kernel, bricks, members, halves, sizes, pooled),
        out_shape=outs,
        in_specs=[ANY] * 4 + [VMEM] + [ANY] * len(pieces) + [VMEM] * len(held),
        out_specs=[VMEM] * len(outs),
        scratch_shapes=[
            pltpu.VMEM((sum(sizes) + 1, 64, 128), BF16),
            pltpu.VMEM((512, 128), BF16),
            pltpu.VMEM((COMPACT, 128), BF16),
            pltpu.VMEM((COMPACT, channels), F32),
            pltpu.VMEM((800, channels), F32),
            pltpu.VMEM((160, channels), F32),
            pltpu.VMEM((160, channels), F32),
            pltpu.VMEM((640, 9 * channels), BF16),
            *[pltpu.SMEM(value.shape, value.dtype) for value in (here, links, sends, places)],
            pltpu.SemaphoreType.DMA((4 + len(pieces),)),
        ],
        compiler_params=grant(sum(sizes) * 33_000 + channels * 90_000),
        name="level" + str(channels),
    )(here, links, sends, places, gain[None, :], *pieces, *held)


def per_device(
    nx, ny,
    voxels_fine, gain_fine, gain_middle, gain_coarse, kernel_fine, kernel_middle, kernel_coarse,
    lift_middle, lift_coarse, links_fine, links_middle, links_coarse, sends_fine, sends_middle,
    sends_coarse, parents_middle, parents_coarse, uplinks_middle, uplinks_coarse,
):
    members = nx * ny
    bricks0, bricks1, bricks2 = voxels_fine.shape[0], links_middle.shape[0], links_coarse.shape[0]
    pairs = bricks0 // 2
    pool = pool_matrix()

    mx, my = lax.axis_index("gx"), lax.axis_index("gy")
    here = jnp.stack([mx * ny + my, mx, my])[None].astype(jnp.int32)
    assert members + bricks0 <= 256 and 6 * bricks1 <= 256
    width = sum(
        table.shape[-1]
        for table in (sends_middle.reshape(members, -1), sends_coarse.reshape(members, -1), uplinks_middle, uplinks_coarse)
    ) + 8 * (bricks1 + bricks2)
    size = -(-width // 1024) * 8
    slots = sends_fine.shape[1] // members

    indices = (
        sends_fine, sends_middle, sends_coarse, parents_middle, parents_coarse, uplinks_middle, uplinks_coarse,
    )
    act, faces, outgoing = pl.pallas_call(
        functools.partial(pack_kernel, pairs, slots),
        out_shape=[
            jax.ShapeDtypeStruct((pairs, 512, 128), BF16),
            jax.ShapeDtypeStruct((12 * pairs + 1, 32, 128), BF16),
            jax.ShapeDtypeStruct((members, 32 * slots + size, 128), BF16),
        ],
        in_specs=[ANY] * 7 + [ANY, VMEM],
        out_specs=[HBM] * 3,
        scratch_shapes=[
            *[pltpu.SMEM(value.shape, value.dtype) for value in indices],
            pltpu.VMEM(voxels_fine.shape, BF16),
            pltpu.VMEM((pairs, 512, 128), BF16),
            pltpu.VMEM((12 * pairs + 1, 32, 128), BF16),
            pltpu.VMEM((members, 32 * slots + size, 128), BF16),
            pltpu.VMEM((512, 128), F32),
            pltpu.SemaphoreType.DMA((8,)),
            pltpu.SemaphoreType.DMA((4,)),
            pltpu.SemaphoreType.DMA((2,)),
        ],
        compiler_params=grant(WHOLE),
        name="pack",
    )(*indices, voxels_fine, gain_fine[None])

    outgoing, act, kernel_fine, kernel_middle, kernel_coarse = lax.optimization_barrier(
        (outgoing, act, kernel_fine, kernel_middle, kernel_coarse)
    )
    arrived = lax.all_to_all(outgoing, AXES, split_axis=0, concat_axis=0, tiled=True)

    slots1, slots2 = sends_middle.shape[1] // members, sends_coarse.shape[1] // members
    levels = ((bricks1, slots1, bricks0, 2), (bricks2, slots2, bricks1, 1))
    def columns(kernel):
        return kernel.transpose(0, 2, 1).reshape(3, 9 * kernel.shape[2], kernel.shape[1])

    def side_by_side(kernel):
        first = jnp.concatenate([kernel[0], kernel[1]], axis=1)
        return jnp.stack([first, jnp.concatenate([kernel[2], jnp.zeros_like(kernel[2])], axis=1)])

    turned = kernel_fine.transpose(0, 2, 1)
    blank = jnp.zeros_like(turned)
    kernel0 = jnp.concatenate(
        [jnp.concatenate([turned, blank], axis=2), jnp.concatenate([blank, turned], axis=2)], axis=1
    ).reshape(3, 9 * 128, 128)
    kernel1, kernel2 = columns(kernel_middle), columns(kernel_coarse)
    kernel1 = side_by_side(kernel1)
    lift1 = jnp.concatenate([lift_middle.T, lift_middle.T], axis=0)
    lift2 = lift_coarse.T
    cube = kernel0.reshape(3, 3, 3, 128, 128)
    rim0 = jnp.stack(
        [part.reshape(9 * 128, 128) for at in ((0,), (slice(None), 0), (slice(None), slice(None), 0))
         for part in (cube[at], cube[at[:-1] + (2,)])]
    )
    inner = pl.pallas_call(
        functools.partial(inner_kernel, pairs),
        out_shape=jax.ShapeDtypeStruct((pairs, 512, 128), F32),
        in_specs=[HBM] * 2,
        out_specs=VMEM,
        scratch_shapes=[
            pltpu.VMEM(act.shape, BF16),
            pltpu.VMEM((2, 9 * 128, 256), BF16),
            pltpu.VMEM((800, 128), F32),
            pltpu.VMEM((160, 128), F32),
            pltpu.VMEM((160, 128), F32),
            pltpu.VMEM((640, 9 * 128), BF16),
            pltpu.SemaphoreType.DMA((2,)),
        ],
        compiler_params=grant(WHOLE),
        name="inner",
    )(act, side_by_side(kernel0))
    arrived, inner, rim0, kernel1, kernel2, lift1, lift2 = lax.optimization_barrier(
        (arrived, inner, rim0, kernel1, kernel2, lift1, lift2)
    )

    output_fine, pooled_fine = pl.pallas_call(
        functools.partial(fine_kernel, pairs),
        out_shape=[
            jax.ShapeDtypeStruct(voxels_fine.shape, BF16),
            jax.ShapeDtypeStruct((pairs, 64, 128), BF16),
        ],
        in_specs=[ANY] + [HBM] * 6,
        out_specs=[VMEM] * 2,
        scratch_shapes=[
            pltpu.SMEM(links_fine.shape, jnp.int32),
            *[pltpu.VMEM(value.shape, value.dtype) for value in (arrived, faces, inner, rim0, voxels_fine, pool)],
            pltpu.VMEM((64 * WAYS, 128), F32),
            pltpu.VMEM((6, 64 * pairs, 9 * 128), BF16),
            pltpu.VMEM((6, 64 * pairs, 128), F32),
            pltpu.SemaphoreType.DMA((7,)),
        ],
        compiler_params=grant(WHOLE),
        name="fine",
    )(links_fine, arrived, faces, inner, rim0, voxels_fine, pool)

    consts = (place_matrix(), face_matrices(), *rim_matrices(), pool, half_masks())
    table = arrived[:, 32 * slots :].reshape(members, -1)[:, :width].astype(F32).astype(jnp.int32)
    places1, here1, places2, here2 = pl.pallas_call(
        functools.partial(places_kernel, nx, ny, levels),
        out_shape=[
            jax.ShapeDtypeStruct(shape, jnp.int32)
            for bricks, slots_, _, _ in levels
            for shape in ((8 * bricks, members), (members, slots_))
        ],
        in_specs=[SMEM, VMEM],
        out_specs=[VMEM] * 4,
        compiler_params=grant(4_000_000),
        name="places",
    )(here, table)
    blocks, (places1, here1, places2, here2) = gather_blocks(
        pooled_fine, nx, ny, (places1, here1, places2, here2)
    )
    output_middle, pooled_middle = run_level(
        here, links_middle, here1, places1, blocks, gain_middle, lift1, kernel1,
        members, 2, True, consts,
    )
    (output_coarse,) = run_level(
        here, links_coarse, here2, places2, gather_blocks(pooled_middle, nx, ny, ())[0], gain_coarse, lift2, kernel2,
        members, 1, False, consts,
    )
    return (output_fine, output_middle, output_coarse)


def solution(mesh):
    nx, ny = mesh.shape["gx"], mesh.shape["gy"]
    split3, split2, whole = P(AXES, None, None), P(AXES, None), P()
    return jax.shard_map(
        functools.partial(per_device, nx, ny),
        mesh=mesh,
        in_specs=(split3,) + (whole,) * 8 + (split2,) * 10,
        out_specs=(split3,) * 3,
        check_vma=False,
    )
```
